32 devices in a mesh: fx: 4 (over z), fy: 4 (over x, core), fz: 2 (over y).
Axes of the slice: x: 2, y: 2, z: 4, core: 2. Of those that a mesh axis runs over, the one named last changes fastest.
Arguments:
- pressure: float32 [128, 512, 256], P('fx', 'fy', 'fz'), may hold values from -6 to 6
- source: float32 [128, 512, 256], P('fx', 'fy', 'fz'), may hold values from -6 to 6
- diag_shift: float32 [128, 512, 256], P('fx', 'fy', 'fz'), may hold values from 0.1 to 2
- iface_cells: int32 [262144], P(('fx', 'fy', 'fz')), may hold values from 0 to 524287
- iface_coef: float32 [262144], P(('fx', 'fy', 'fz')), may hold values from -6 to 6
- iface_xyz: float32 [3, 262144], P(None, ('fx', 'fy', 'fz')), may hold values from -6 to 6
- node_xyz: float32 [3, 65536], P(None, ('fx', 'fy', 'fz')), may hold values from -6 to 6
- owners: int32 [2048], P(('fx', 'fy', 'fz')), may hold values from 0 to 31, as said below
- node_lists: int32 [65536, 8], P(('fx', 'fy', 'fz')), may hold values from 0 to 1048575
Outputs:
- new_pressure: float32 [128, 512, 256], P('fx', 'fy', 'fz')
- node_loads: float32 [65536], P(('fx', 'fy', 'fz'))
The draws below stay inside these ranges and needn't reach their ends.
Inputs may be any that keep to these rules, and one draw needn't show every extreme that they name: `owners`: among the 64 tiles of one device, at most 4 have the same owner; one device owns exactly 4 tiles of every device's block; every device owns at least one tile.
All inputs are finite; a program needn't handle non-finite values.
Results may differ from the reference program's by a relative error of at most 0.0003.
Values sent between devices are 32-bit elements; how exact they have to be, the bound alone decides.
A program may use at most 192 MiB of HBM per device.

```python
import math
import jax
import jax.numpy as jnp
from jax import lax

CX = 32
CY = 128
CZ = 128
ITERS = 4
TILE = 128
CAP = 4
NODE_DEV = 2048
NEIGH = 8
OWNERS = 32
TILES_DEV = 64
NX = 128
NY = 512
NZ = 256
NTILES = 2048
NPTS = 262144
NODES = 65536
N_FY = 4
N_FZ = 2


def draw_owners(key, part):
    key_heavy, key_jitter, key_order = jax.random.split(jax.random.fold_in(key, 7031), 3)
    heavy = jax.random.randint(key_heavy, (), 0, OWNERS)
    jitter = jax.random.randint(key_jitter, (OWNERS,), 0, CAP)
    cycle_len = (OWNERS - 1) * CAP
    window = TILES_DEV - CAP
    senders = jnp.arange(OWNERS, dtype=jnp.int32)
    starts = senders * window + jitter
    spots = (starts[:, None] + jnp.arange(window, dtype=jnp.int32)[None, :]) % cycle_len
    others = (heavy + 1 + spots // CAP) % OWNERS
    heavy_part = jnp.zeros((OWNERS, CAP), jnp.int32) + heavy
    table = jnp.concatenate([heavy_part, others.astype(jnp.int32)], axis=1)
    scores = jax.random.randint(key_order, (OWNERS, TILES_DEV), 0, 1048576) * TILES_DEV
    scores = scores + jnp.arange(TILES_DEV, dtype=jnp.int32)[None, :]
    shuffle = jnp.argsort(scores, axis=1, stable=True)
    table = jnp.take_along_axis(table, shuffle, axis=1)
    return table.reshape(-1).astype(jnp.int32)


def set_ends(drawn, own_key, smallest, high):
    longest = drawn.shape.index(max(drawn.shape))
    spots = []
    for shift in (0, 1):
        where = [jax.random.randint(jax.random.fold_in(own_key, axis), (), 0, length) for axis, length in enumerate(drawn.shape)]
        where[longest] = (where[longest] + shift) % drawn.shape[longest]
        spots.append(tuple(where))
    return drawn.at[spots[0]].set(smallest).at[spots[1]].set(high)


def block_levels(own_key, dims, cuts, least, largest):
    level, own = 1.0, jax.random.fold_in(own_key, 6)
    for axis_at, shards_of in cuts:
        heights = jnp.exp(jax.random.uniform(jax.random.fold_in(own, axis_at), (shards_of,), jnp.float32, least / len(cuts), largest / len(cuts)))
        level = level * jnp.repeat(heights, dims[axis_at] // shards_of).reshape([-1 if axis == axis_at else 1 for axis in range(len(dims))])
    return level


def noise(rng, dims, spread, most, cuts=(), kind=jnp.bfloat16):
    array = jax.random.normal(rng, dims, jnp.float32) * spread
    if len(cuts) > 0:
        array = block_levels(rng, dims, cuts, -0.22, 0.18) * array
    return jnp.clip(array, min=-most, max=most).astype(kind)


def setup_inputs(seed: int = 0) -> dict:
    key_of = jax.random.split(jax.random.key(seed), 10)
    pressure = noise(key_of[0], (NX, NY, NZ), 1.0, 6.0, ((0, 4), (1, 4), (2, 2)), jnp.float32)
    source = noise(key_of[1], (NX, NY, NZ), 1.0, 6.0, ((0, 4), (1, 4), (2, 2)), jnp.float32)
    diag_shift = jnp.clip(jnp.exp(math.log(2.0) - 2.9957323 * jax.random.uniform(key_of[2], (NX, NY, NZ), jnp.float32) ** block_levels(key_of[2], (NX, NY, NZ), ((0, 4), (1, 4), (2, 2)), -0.2, 0.2)), 0.1, 2.0)
    iface_cells = set_ends(jax.random.randint(key_of[3], (NPTS,), 0, CX * CY * CZ), jax.random.fold_in(key_of[3], 1), 0, (CX * CY * CZ) - 1).astype(jnp.int32)
    iface_coef = noise(key_of[4], (NPTS,), 1.0, 6.0, ((0, 32),), jnp.float32)
    iface_xyz = noise(key_of[5], (3, NPTS), 1.0, 6.0, ((1, 32),), jnp.float32)
    node_xyz = noise(key_of[6], (3, NODES), 1.0, 6.0, ((1, 32),), jnp.float32)
    owners = draw_owners(jax.random.fold_in(key_of[9], 71), 0)
    node_lists = set_ends(jax.random.randint(key_of[8], (NODES, NEIGH), 0, 1048576), jax.random.fold_in(key_of[8], 1), 0, 1048575).astype(jnp.int32)
    return dict(pressure=pressure, source=source, diag_shift=diag_shift, iface_cells=iface_cells, iface_coef=iface_coef, iface_xyz=iface_xyz, node_xyz=node_xyz, owners=owners, node_lists=node_lists)


GAUSS_RATE = 0.5


def jacobi_step(pressure_now, source, diag_shift):
    neighbours = jnp.roll(pressure_now, 1, 0) + jnp.roll(pressure_now, -1, 0)
    neighbours = neighbours + jnp.roll(pressure_now, 1, 1) + jnp.roll(pressure_now, -1, 1)
    neighbours = neighbours + jnp.roll(pressure_now, 1, 2) + jnp.roll(pressure_now, -1, 2)
    return (neighbours + source) / (6.0 + diag_shift)


def reference(pressure, source, diag_shift, iface_cells, iface_coef, iface_xyz, node_xyz, owners, node_lists):
    points = jnp.arange(NPTS, dtype=jnp.int32)
    holder = points // (TILES_DEV * TILE)
    block_x = holder // (N_FY * N_FZ)
    block_y = (holder // N_FZ) % N_FY
    block_z = holder % N_FZ
    cell_x = block_x * CX + iface_cells // (CY * CZ)
    cell_y = block_y * CY + (iface_cells // CZ) % CY
    cell_z = block_z * CZ + iface_cells % CZ
    values = iface_coef * pressure[cell_x, cell_y, cell_z]
    pressure_now = pressure
    for sweep_index in range(ITERS):
        pressure_now = jacobi_step(pressure_now, source, diag_shift)
    counts = jnp.bincount(owners, length=OWNERS).astype(jnp.int32)
    grouped = jnp.argsort(owners, stable=True).astype(jnp.int32)
    offsets = (jnp.cumsum(counts) - counts).astype(jnp.int32)
    tile_values = values.reshape(NTILES, TILE)
    tile_xyz = iface_xyz.reshape(3, NTILES, TILE)

    def one_owner(inputs):
        owner_id, coords, entries = inputs
        chosen = grouped[offsets[owner_id] + entries % counts[owner_id]]
        distance = jnp.zeros((NODE_DEV, NEIGH, TILE), jnp.float32)
        for component in range(3):
            gap_axis = coords[component][:, None, None] - tile_xyz[component][chosen]
            distance = distance + gap_axis * gap_axis
        return jnp.sum(jnp.exp(-GAUSS_RATE * distance) * tile_values[chosen], axis=(1, 2))

    owner_ids = jnp.arange(OWNERS, dtype=jnp.int32)
    node_coords = node_xyz.reshape(3, OWNERS, NODE_DEV).transpose(1, 0, 2)
    node_entries = node_lists.reshape(OWNERS, NODE_DEV, NEIGH)
    node_loads = lax.map(one_owner, (owner_ids, node_coords, node_entries))
    return pressure_now, node_loads.reshape(NODES)
```

```python
import functools
import math

import jax
import jax.numpy as jnp
from jax import lax
from jax.experimental import pallas as pl
from jax.experimental.pallas import tpu as pltpu
from jax.sharding import PartitionSpec as P

ITERS = 4
CAP = 4
GAUSS_RATE = 0.5
SCALE = math.sqrt(GAUSS_RATE * math.log2(math.e))
FAR = 1.0e6
NODE_BLOCK = 256
ROWS = 32
GROUP = 16
PAD = 8
MESH = pl.DeviceIdType.MESH
F32 = jnp.float32
BF16 = jnp.bfloat16


def split2(x):
    hi = x.astype(BF16)
    return hi, (x - hi.astype(F32)).astype(BF16)


def split3(x):
    hi = x.astype(BF16)
    rest = x - hi.astype(F32)
    mid = rest.astype(BF16)
    return hi, mid, (rest - mid.astype(F32)).astype(BF16)


def mm(a, b):
    return jnp.dot(a, b, preferred_element_type=F32)


def iota(shape, dim):
    return lax.broadcasted_iota(jnp.int32, shape, dim)


def ones_where(mask):
    return jnp.where(mask, 1.0, 0.0).astype(BF16)


def main_kernel(
    sizes, gauss_bounds,
    p_any, s_any, d_any, cells_any, coef_any, xyz_any, own_any, nodes_any, lists_any,
    new_p, loads,
    a_buf, b_buf, src, inv, hx, hy, hz, ys, zs,
    cells, lanes_v, rows_v, rows_s, coef, xyz, own_v, nodes, lists,
    picked, parts, values, outgoing, incoming, tab, pos, want,
    load_sem, x_send, x_recv, y_send, y_recv, z_send, z_recv, t_send, t_recv,
):
    nfx, nfy, nfz = sizes
    devices = nfx * nfy * nfz
    cx, cy, cz = src.shape
    tiles, width = coef.shape
    bx, by, bz = lax.axis_index("fx"), lax.axis_index("fy"), lax.axis_index("fz")
    me = (bx * nfy + by) * nfz + bz
    body = pl.ds(PAD, cy)

    def local(a, b, k):
        return pltpu.make_async_copy(a, b, load_sem.at[k])

    load_cells = local(cells_any, cells, 0)
    load_p = local(p_any, a_buf.at[:, body, :], 1)
    load_own = local(own_any, own_v, 2)
    load_xyz = local(xyz_any, xyz, 3)
    load_coef = local(coef_any, coef, 4)
    load_d = local(d_any, inv, 5)
    load_s = local(s_any, src, 6)
    load_nodes = local(nodes_any, nodes, 7)
    load_lists = local(lists_any, lists, 8)
    for c in (
        load_cells, load_p, load_own, load_xyz, load_coef,
        load_d, load_s, load_nodes, load_lists,
    ):
        c.start()

    tx = [(bx + d) % nfx for d in range(nfx)]
    ty = [(by + d) % nfy for d in range(nfy)]
    tz = [(bz + d) % nfz for d in range(nfz)]

    def others(act):
        def inner(x_to, first, base):
            for dy in range(nfy):
                for dz in range(nfz):
                    if first and dy == 0 and dz == 0:
                        continue
                    to = (x_to * nfy + ty[dy]) * nfz + tz[dz]
                    act(base + dy * nfz + dz, to, (x_to, ty[dy], tz[dz]))

        inner(tx[0], True, 0)

        def step(d, carry):
            inner((bx + d) % nfx, False, d * (nfy * nfz))
            return carry

        lax.fori_loop(1, nfx, step, 0)

    barrier = pltpu.get_barrier_semaphore()

    def greet(o, to, where):
        pl.semaphore_signal(barrier, inc=1, device_id=where, device_id_type=MESH)

    others(greet)

    def remote(a, b, ss, rs, device):
        return pltpu.make_async_remote_copy(
            src_ref=a, dst_ref=b, send_sem=ss, recv_sem=rs, device_id=device, device_id_type=MESH
        )

    def tile_copy(half, o, to, where):
        return remote(
            outgoing.at[half, to], incoming.at[half, me],
            t_send.at[half, o], t_recv.at[half, o], where,
        )

    x_next, x_prev = (tx[1 % nfx], by, bz), (tx[nfx - 1], by, bz)
    y_next, y_prev = (bx, ty[1 % nfy], bz), (bx, ty[nfy - 1], bz)
    z_next, z_prev = (bx, by, tz[1 % nfz]), (bx, by, tz[nfz - 1])

    def x_copies(it, buf):
        return [
            remote(buf.at[cx - 1, body], hx.at[it, 0], x_send.at[it, 0], x_recv.at[it, 0], x_next),
            remote(buf.at[0, body], hx.at[it, 1], x_send.at[it, 1], x_recv.at[it, 1], x_prev),
        ]

    def start_x(copies):
        @pl.when(bx == 0)
        def _():
            copies[1].start()
            copies[0].start()

        @pl.when(bx != 0)
        def _():
            copies[0].start()
            copies[1].start()

    def yz_copies(it):
        made = [
            remote(zs.at[it], hz.at[it, 0], z_send.at[it, 0], z_recv.at[it, 0], z_next),
            remote(ys.at[it, 1], hy.at[it, 0], y_send.at[it, 0], y_recv.at[it, 0], y_next),
            remote(ys.at[it, 0], hy.at[it, 1], y_send.at[it, 1], y_recv.at[it, 1], y_prev),
        ]
        if nfz > 2:
            made.append(
                remote(zs.at[it], hz.at[it, 1], z_send.at[it, 1], z_recv.at[it, 1], z_prev)
            )
        return made

    full_lane = iota((cy, cz), 1)
    lane = iota((ROWS, cz), 1)
    pair = lax.shift_right_logical(lane, 1)

    load_cells.wait()
    flat = cells[...]
    row_of = lax.shift_right_logical(flat, cz.bit_length() - 1)
    plane_of = lax.shift_right_logical(row_of, cy.bit_length() - 1)
    rows_v[...] = row_of + plane_of * (2 * PAD) + PAD
    lanes_v[...] = jnp.bitwise_and(flat, cz - 1)

    def send_rows(it, buf):
        def one(x, carry):
            ys[it, 0, pl.ds(x, 1), :] = buf[x, pl.ds(PAD, 1), :]
            ys[it, 1, pl.ds(x, 1), :] = buf[x, pl.ds(PAD + cy - 1, 1), :]
            return carry

        lax.fori_loop(0, cx, one, 0, unroll=8)

    load_p.wait()

    def first_faces(yb, carry):
        y0 = pl.multiple_of(yb * ROWS, ROWS)
        packed = jnp.zeros((ROWS, cz), F32)
        for x in range(cx):
            plane = a_buf[x, pl.ds(y0 + PAD, ROWS), :]
            packed = jnp.where(pair == x, pltpu.roll(plane, (2 * x + 1) % cz, 1), packed)
        zs[0, pl.ds(y0, ROWS), :] = packed
        return carry

    lax.fori_loop(0, cy // ROWS, first_faces, 0)
    send_rows(0, a_buf)

    load_rows = pltpu.make_async_copy(rows_v, rows_s, load_sem.at[0])
    load_rows.start()

    pl.semaphore_wait(barrier, devices - 1)
    started = [x_copies(0, a_buf)]
    start_x(started[0])
    started[0] = started[0] + yz_copies(0)
    for c in started[0][2:]:
        c.start()

    load_own.wait()
    own = own_v[...]
    mine = iota((devices, tiles), 0) == own
    before = ones_where(iota((tiles, tiles), 0) < iota((tiles, tiles), 1))
    earlier = mm(ones_where(mine), before)
    rank = jnp.sum(jnp.where(mine, earlier, 0.0), axis=0, keepdims=True)
    target = own * CAP + rank.astype(jnp.int32)
    line = iota((devices * 8, tiles), 0)
    at_slot = (line // 8) * CAP + line % CAP == target
    low_rows = line % 8 < CAP
    first = ones_where(at_slot & low_rows)
    second = ones_where(at_slot & jnp.logical_not(low_rows))
    filled = mm(first, jnp.ones((tiles, width), BF16))

    load_xyz.wait()

    def spread(t, carry):
        base = pl.multiple_of(t * width, width)
        for c in range(3):
            parts[c, pl.ds(t, 1), :] = xyz[c : c + 1, pl.ds(base, width)]
        return carry

    lax.fori_loop(0, tiles, spread, 0, unroll=8)

    def placed(pairs):
        total = None
        for sel, block in pairs:
            for piece in split3(block):
                term = mm(sel, piece)
                total = term if total is None else total + term
        return total

    total = placed(((first, parts[0]), (second, parts[1])))
    empty = (iota(filled.shape, 0) % 8 < CAP) & (filled < 0.5)
    outgoing[0] = jnp.where(empty, FAR, total).reshape(devices, 8, width)
    others(lambda o, to, where: tile_copy(0, o, to, where).start())
    incoming[0, me] = outgoing[0, me]

    load_rows.wait()
    table = a_buf.reshape(cx * (cy + 2 * PAD), cz)
    blocks = width // GROUP

    def fetch(g, slot):
        row0, col0 = (g // blocks) * 8, (g % blocks) * GROUP
        for s in range(8):
            for j in range(GROUP):
                at = rows_s[row0 + s, col0 + j]
                picked[slot, j, s : s + 1, :] = table[pl.ds(at, 1), :]

    def pick(g, slot):
        span = pl.ds(pl.multiple_of((g // blocks) * 8, 8), 8)
        lanes = lanes_v[span, :]
        rel = iota((8, width), 1) - (g % blocks) * GROUP
        out = values[span, :]
        for j in range(GROUP):
            got = jnp.take_along_axis(picked[slot, j], lanes, axis=1)
            out = jnp.where(rel == j, got, out)
        values[span, :] = out

    groups = (tiles // 8) * blocks
    values[...] = jnp.zeros((tiles, width), F32)
    fetch(0, 0)

    def gather(g, carry):
        pick(g - 1, (g - 1) % 2)
        fetch(g, g % 2)
        return carry

    lax.fori_loop(1, groups, gather, 0)
    pick(groups - 1, (groups - 1) % 2)
    load_coef.wait()
    total = placed(((first, parts[2]), (second, values[...] * coef[...])))
    outgoing[1] = total.reshape(devices, 8, width)
    others(lambda o, to, where: tile_copy(1, o, to, where).start())
    incoming[1, me] = outgoing[1, me]

    load_d.wait()

    def invert(x, carry):
        inv[x] = 1.0 / (6.0 + inv[x])
        return carry

    lax.fori_loop(0, cx, invert, 0, unroll=2)
    load_s.wait()

    def sweep(it, cur, nxt):
        last = it == ITERS - 1
        for c in started[it]:
            c.wait_recv()
        if 0 < it < ITERS - 1:
            for c in started[it - 1][:2]:
                c.wait_send()

        def rows(x, carry):
            cur[x, pl.ds(PAD - 1, 1), :] = hy[it, 0, pl.ds(x, 1), :]
            cur[x, pl.ds(PAD + cy, 1), :] = hy[it, 1, pl.ds(x, 1), :]
            return carry

        lax.fori_loop(0, cx, rows, 0, unroll=8)
        if nfz > 2:
            hz[it, 0] = jnp.where(full_lane % 2 == 0, hz[it, 0], hz[it, 1])

        def plane(x, y0, count, edges, below, mid, above, packed):
            at_lane = iota((count, cz), 1)
            edge = pltpu.roll(edges, (cz - 1 - 2 * x) % cz, 1)
            total = pltpu.roll(jnp.where(at_lane == 0, edge, mid), cz - 1, 1)
            total = total + pltpu.roll(jnp.where(at_lane == cz - 1, edge, mid), 1, 1)
            total = total + cur[x, pl.ds(y0 + (PAD - 1), count), :]
            total = total + cur[x, pl.ds(y0 + (PAD + 1), count), :]
            new = (total + below + above + src[x, pl.ds(y0, count), :]) * inv[x, pl.ds(y0, count), :]
            if last:
                new_p[x, pl.ds(y0, count), :] = new
                return packed
            nxt[x, pl.ds(y0 + PAD, count), :] = new
            at_pair = lax.shift_right_logical(at_lane, 1)
            return jnp.where(at_pair == x, pltpu.roll(new, (2 * x + 1) % cz, 1), packed)

        def at(x, y0, count):
            return cur[x, pl.ds(y0 + PAD, count), :]

        packed = jnp.zeros((cy, cz), F32)
        packed = plane(0, 0, cy, hz[it, 0], hx[it, 0], at(0, 0, cy), at(1, 0, cy), packed)
        packed = plane(
            cx - 1, 0, cy, hz[it, 0], at(cx - 2, 0, cy), at(cx - 1, 0, cy), hx[it, 1], packed
        )
        if not last:
            started.append(x_copies(it + 1, nxt))
            start_x(started[-1])
            zs[it + 1] = packed

        def inner(yb, carry):
            y0 = pl.multiple_of(yb * ROWS, ROWS)
            span = pl.ds(y0, ROWS)
            edges = hz[it, 0, span, :]
            block = zs[it + 1, span, :] if not last else None
            below, mid = at(0, y0, ROWS), at(1, y0, ROWS)
            for x in range(1, cx - 1):
                above = at(x + 1, y0, ROWS)
                block = plane(x, y0, ROWS, edges, below, mid, above, block)
                below, mid = mid, above
            if not last:
                zs[it + 1, span, :] = block
            return carry

        lax.fori_loop(0, cy // ROWS, inner, 0)
        if not last:
            more = yz_copies(it + 1)
            more[0].start()
            send_rows(it + 1, nxt)
            for c in more[1:]:
                c.start()
            started[-1] = started[-1] + more

    slots = devices * CAP
    lines = devices * 8

    def prepare():
        for half in range(2):
            others(lambda o, to, where: tile_copy(half, o, to, where).wait_recv())
        load_lists.wait()
        low = incoming[0].reshape(lines, width)
        high = incoming[1].reshape(lines, width)
        row = iota((lines, slots), 0)
        col = iota((lines, slots), 1)
        home = (row // 8) * CAP + row % CAP
        lower = row % 8 < CAP
        take = (ones_where((home == col) & lower), ones_where((home == col) & (row % 8 >= CAP)))
        for half, block in ((0, low), (1, high)):
            turned = block.T
            for odd in range(2):
                c = 2 * half + odd
                scaled = turned if c == 3 else turned * SCALE
                hi, lo = split2(scaled)
                span = pl.ds(c * width, width)
                tab[span, 0:slots] = mm(hi, take[odd]).astype(BF16)
                tab[span, slots : 2 * slots] = mm(lo, take[odd]).astype(BF16)
        here = ones_where(low < 0.5 * FAR)
        row = iota((slots, lines), 0)
        col = iota((slots, lines), 1)
        home = (col // 8) * CAP + col % CAP
        lower = col % 8 < CAP
        prefix = mm(ones_where((home <= row) & lower), here)
        there = mm(ones_where((home == row) & lower), here)
        place = jnp.where(there > 0.5, prefix - 1.0, -1.0)
        pos[:, 0:width] = place
        pos[:, width : 2 * width] = place
        count = prefix[slots - 1 : slots, 0:1]
        entry = lists[...].astype(F32)
        rest = entry - jnp.floor(entry / count) * count
        rest = jnp.where(rest < 0.0, rest + count, rest)
        want[...] = jnp.where(rest >= count, rest - count, rest)
        load_nodes.wait()

    neigh = lists.shape[0]

    def gauss(block, carry):
        span = pl.ds(pl.multiple_of(block * NODE_BLOCK, NODE_BLOCK), NODE_BLOCK)
        here = [nodes[c : c + 1, span] * SCALE for c in range(3)]
        total = jnp.zeros((8, NODE_BLOCK), F32)
        for k in range(neigh):
            hot = ones_where(pos[...] == want[k : k + 1, span])
            hot = jnp.concatenate([hot, hot], axis=0)
            got = mm(tab[...], hot)
            far = None
            for c in range(3):
                gap = got[c * width : (c + 1) * width] - here[c]
                far = gap * gap if far is None else far + gap * gap
            term = jnp.exp2(-far) * got[3 * width : 4 * width]
            total = total + jnp.sum(term.reshape(width // 8, 8, NODE_BLOCK), axis=0)
        done = jnp.sum(total, axis=0, keepdims=True)
        for h in range(NODE_BLOCK // 128):
            loads[pl.ds(block * (NODE_BLOCK // 128) + h, 1), :] = done[:, h * 128 : (h + 1) * 128]
        return carry

    bufs = (a_buf, b_buf)
    for it in range(ITERS):
        if it == ITERS - 1:
            for group in started[:-1]:
                for c in group[2:]:
                    c.wait_send()
            for c in started[-2][:2] + started[-1]:
                c.wait_send()
            for half in range(2):
                others(lambda o, to, where: tile_copy(half, o, to, where).wait_send())
        sweep(it, bufs[it % 2], bufs[(it + 1) % 2])
        if it == 0:
            prepare()
        if it < ITERS - 1:
            lax.fori_loop(gauss_bounds[it], gauss_bounds[it + 1], gauss, 0)


def on_device(
    sizes,
    pressure, source, diag_shift, iface_cells, iface_coef, iface_xyz, node_xyz, owners, node_lists,
):
    nfx, nfy, nfz = sizes
    devices = nfx * nfy * nfz
    tiles = owners.shape[0]
    width = iface_coef.shape[0] // tiles
    cx, cy, cz = pressure.shape
    nodes, neigh = node_lists.shape
    vmem = pl.BlockSpec(memory_space=pltpu.VMEM)
    hbm = pl.BlockSpec(memory_space=pltpu.HBM)
    slots = devices * CAP
    blocks = nodes // NODE_BLOCK
    bounds = [blocks * i // (ITERS - 1) for i in range(ITERS)]
    dma = pltpu.SemaphoreType.DMA

    def space(*shape, dtype=F32):
        return pltpu.VMEM(shape, dtype)

    new_p, loads = pl.pallas_call(
        functools.partial(main_kernel, sizes, bounds),
        out_shape=(
            jax.ShapeDtypeStruct((cx, cy, cz), F32),
            jax.ShapeDtypeStruct((nodes // 128, 128), F32),
        ),
        in_specs=[hbm] * 9,
        out_specs=(vmem, vmem),
        scratch_shapes=[
            space(cx, cy + 2 * PAD, cz),
            space(cx, cy + 2 * PAD, cz),
            space(cx, cy, cz),
            space(cx, cy, cz),
            space(ITERS, 2, cy, cz),
            space(ITERS, 2, cx, cz),
            space(ITERS, 2, cy, cz),
            space(ITERS, 2, cx, cz),
            space(ITERS, cy, cz),
            space(tiles, width, dtype=jnp.int32),
            space(tiles, width, dtype=jnp.int32),
            space(tiles, width, dtype=jnp.int32),
            pltpu.SMEM((tiles, width), jnp.int32),
            space(tiles, width),
            space(3, tiles * width),
            space(1, tiles, dtype=jnp.int32),
            space(3, nodes),
            space(neigh, nodes, dtype=jnp.int32),
            space(2, GROUP, 8, width),
            space(3, tiles, width),
            space(tiles, width),
            space(2, devices, 8, width),
            space(2, devices, 8, width),
            space(4 * width, 2 * slots, dtype=BF16),
            space(slots, NODE_BLOCK),
            space(neigh, nodes),
            dma((9,)),
            dma((ITERS, 2)), dma((ITERS, 2)),
            dma((ITERS, 2)), dma((ITERS, 2)),
            dma((ITERS, 2)), dma((ITERS, 2)),
            dma((2, devices)), dma((2, devices)),
        ],
        compiler_params=pltpu.CompilerParams(
            collective_id=0, has_side_effects=True, vmem_limit_bytes=28 * 1024 * 1024
        ),
        name="sweeps",
    )(
        pressure,
        source,
        diag_shift,
        iface_cells.reshape(tiles, width),
        iface_coef.reshape(tiles, width),
        iface_xyz,
        owners.reshape(1, tiles),
        node_xyz,
        node_lists.T,
    )
    return new_p, loads.reshape(nodes)


def solution(mesh):
    sizes = tuple(mesh.shape[a] for a in ("fx", "fy", "fz"))
    cells = P("fx", "fy", "fz")
    flat = P(("fx", "fy", "fz"))
    return jax.shard_map(
        functools.partial(on_device, sizes),
        mesh=mesh,
        in_specs=(
            cells, cells, cells, flat, flat,
            P(None, ("fx", "fy", "fz")), P(None, ("fx", "fy", "fz")), flat,
            P(("fx", "fy", "fz"), None),
        ),
        out_specs=(cells, flat),
        check_vma=False,
    )
```

```python
import functools
import math

import jax
import jax.numpy as jnp
from jax import lax
from jax.experimental import pallas as pl
from jax.experimental.pallas import tpu as pltpu
from jax.sharding import PartitionSpec as P

ITERS = 4
CAP = 4
GAUSS_RATE = 0.5
SCALE = math.sqrt(GAUSS_RATE * math.log2(math.e))
FAR = 1.0e6
NODE_BLOCK = 256
PLANES = 16
EARLY = 44
PAD = 8
MESH = pl.DeviceIdType.MESH
F32 = jnp.float32
BF16 = jnp.bfloat16


def split2(x):
    hi = x.astype(BF16)
    return hi, (x - hi.astype(F32)).astype(BF16)


def split3(x):
    hi = x.astype(BF16)
    rest = x - hi.astype(F32)
    mid = rest.astype(BF16)
    return hi, mid, (rest - mid.astype(F32)).astype(BF16)


def mm(a, b):
    return jnp.dot(a, b, preferred_element_type=F32)


def iota(shape, dim):
    return lax.broadcasted_iota(jnp.int32, shape, dim)


def ones_where(mask):
    return jnp.where(mask, 1.0, 0.0).astype(BF16)


def main_kernel(
    sizes, gauss_bounds,
    p_any, s_any, d_any, cells_any, coef_any, xyz_any, own_any, nodes_any, lists_any,
    new_p, loads,
    a_buf, b_buf, src, inv, zsum, hx, hy, hz, ys, zs, shift,
    cells, lanes_v, rows_v, rows_s, coef, xyz, own_v, nodes, lists,
    picked, parts, values, outgoing, incoming, tab, pos, want,
    load_sem, x_send, x_recv, y_send, y_recv, z_send, z_recv, t_send, t_recv,
):
    nfx, nfy, nfz = sizes
    devices = nfx * nfy * nfz
    cx, cy, cz = src.shape
    tiles, width = coef.shape
    bx, by, bz = lax.axis_index("fx"), lax.axis_index("fy"), lax.axis_index("fz")
    me = (bx * nfy + by) * nfz + bz
    body = pl.ds(PAD, cy)

    def local(a, b, k):
        return pltpu.make_async_copy(a, b, load_sem.at[k])

    load_cells = local(cells_any, cells, 0)
    load_p = local(p_any, a_buf.at[:, body, :], 1)
    load_own = local(own_any, own_v, 2)
    load_xyz = local(xyz_any, xyz, 3)
    load_coef = local(coef_any, coef, 4)
    load_d = local(d_any, inv, 5)
    load_s = local(s_any, src, 6)
    load_nodes = local(nodes_any, nodes, 7)
    load_lists = local(lists_any, lists, 8)
    for c in (
        load_cells, load_p, load_own, load_xyz, load_coef,
        load_d, load_s, load_nodes, load_lists,
    ):
        c.start()

    tx = [(bx + d) % nfx for d in range(nfx)]
    ty = [(by + d) % nfy for d in range(nfy)]
    tz = [(bz + d) % nfz for d in range(nfz)]

    def others(act):
        def inner(x_to, first, base):
            for dy in range(nfy):
                for dz in range(nfz):
                    if first and dy == 0 and dz == 0:
                        continue
                    to = (x_to * nfy + ty[dy]) * nfz + tz[dz]
                    act(base + dy * nfz + dz, to, (x_to, ty[dy], tz[dz]))

        inner(tx[0], True, 0)

        def step(d, carry):
            inner((bx + d) % nfx, False, d * (nfy * nfz))
            return carry

        lax.fori_loop(1, nfx, step, 0)

    barrier = pltpu.get_barrier_semaphore()

    def greet(o, to, where):
        pl.semaphore_signal(barrier, inc=1, device_id=where, device_id_type=MESH)

    others(greet)

    def remote(a, b, ss, rs, device):
        return pltpu.make_async_remote_copy(
            src_ref=a, dst_ref=b, send_sem=ss, recv_sem=rs, device_id=device, device_id_type=MESH
        )

    def tile_copy(half, o, to, where):
        return remote(
            outgoing.at[half, to], incoming.at[half, me],
            t_send.at[half, o], t_recv.at[half, o], where,
        )

    x_next, x_prev = (tx[1 % nfx], by, bz), (tx[nfx - 1], by, bz)
    y_next, y_prev = (bx, ty[1 % nfy], bz), (bx, ty[nfy - 1], bz)
    z_next, z_prev = (bx, by, tz[1 % nfz]), (bx, by, tz[nfz - 1])

    def x_copies(it, buf):
        return [
            remote(buf.at[cx - 1, body], hx.at[it, 0], x_send.at[it, 0], x_recv.at[it, 0], x_next),
            remote(buf.at[0, body], hx.at[it, 1], x_send.at[it, 1], x_recv.at[it, 1], x_prev),
        ]

    def start_x(copies):
        @pl.when(bx == 0)
        def _():
            copies[1].start()
            copies[0].start()

        @pl.when(bx != 0)
        def _():
            copies[0].start()
            copies[1].start()

    def yz_copies(it):
        made = [
            remote(zs.at[it], hz.at[it, 0], z_send.at[it, 0], z_recv.at[it, 0], z_next),
            remote(ys.at[it, 1], hy.at[it, 0], y_send.at[it, 0], y_recv.at[it, 0], y_next),
            remote(ys.at[it, 0], hy.at[it, 1], y_send.at[it, 1], y_recv.at[it, 1], y_prev),
        ]
        if nfz > 2:
            made.append(
                remote(zs.at[it], hz.at[it, 1], z_send.at[it, 1], z_recv.at[it, 1], z_prev)
            )
        return made

    halves = cz // (2 * cx)
    band = cy // halves
    lane = iota((band, cz), 1)
    pair = lax.shift_right_logical(lane, 1)
    even = lane % 2 == 0
    ends = (lane == 0) | (lane == cz - 1)

    load_cells.wait()
    flat = cells[...]
    row_of = lax.shift_right_logical(flat, cz.bit_length() - 1)
    plane_of = lax.shift_right_logical(row_of, cy.bit_length() - 1)
    rows_v[...] = row_of + plane_of * (2 * PAD) + PAD
    lanes_v[...] = jnp.bitwise_and(flat, cz - 1)

    def send_rows(it, buf):
        def one(x, carry):
            ys[it, 0, pl.ds(x, 1), :] = buf[x, pl.ds(PAD, 1), :]
            ys[it, 1, pl.ds(x, 1), :] = buf[x, pl.ds(PAD + cy - 1, 1), :]
            return carry

        lax.fori_loop(0, cx, one, 0, unroll=8)

    load_p.wait()

    def pack(it, buf):
        def block(half, packed):
            y0 = pl.multiple_of(half * band, band)
            turn = half * (2 * cx)
            for x in range(cx):
                moved = pltpu.roll(buf[x, pl.ds(y0 + PAD, band), :], turn + (2 * x + 1), 1)
                packed = jnp.where(pair == x + half * cx, moved, packed)
            return packed

        packed = lax.fori_loop(0, halves, block, jnp.zeros((band, cz), F32))
        zs[it] = jnp.where(even, packed, pltpu.roll(packed, cz - 2, 1))

    apart = jnp.abs(iota((cz, cz), 0) - iota((cz, cz), 1))
    for part in range(2):
        shift[part * cz : (part + 1) * cz, :] = ones_where(apart == 1)

    def third(buf):
        def block(g, carry):
            span = pl.ds(g * PLANES, PLANES)
            hi, lo = split2(buf[span, body, :].reshape(PLANES * cy, cz))
            near = mm(jnp.concatenate([hi, lo], axis=1), shift[...])
            zsum[span] = near.reshape(PLANES, cy, cz)
            return carry

        lax.fori_loop(0, cx // PLANES, block, 0)

    pack(0, a_buf)
    send_rows(0, a_buf)

    load_rows = pltpu.make_async_copy(rows_v, rows_s, load_sem.at[0])
    load_rows.start()
    third(a_buf)
    load_d.wait()

    def invert(x, carry):
        inv[x] = 1.0 / (6.0 + inv[x])
        return carry

    lax.fori_loop(0, cx, invert, 0, unroll=4)

    pl.semaphore_wait(barrier, devices - 1)
    started = [x_copies(0, a_buf)]
    start_x(started[0])
    started[0] = started[0] + yz_copies(0)
    for c in started[0][2:]:
        c.start()

    load_own.wait()
    own = own_v[...]
    mine = iota((devices, tiles), 0) == own
    before = ones_where(iota((tiles, tiles), 0) < iota((tiles, tiles), 1))
    earlier = mm(ones_where(mine), before)
    rank = jnp.sum(jnp.where(mine, earlier, 0.0), axis=0, keepdims=True)
    target = own * CAP + rank.astype(jnp.int32)
    line = iota((devices * 8, tiles), 0)
    at_slot = (line // 8) * CAP + line % CAP == target
    low_rows = line % 8 < CAP
    first = ones_where(at_slot & low_rows)
    second = ones_where(at_slot & jnp.logical_not(low_rows))
    filled = mm(first, jnp.ones((tiles, width), BF16))

    load_xyz.wait()

    def spread(t, carry):
        base = pl.multiple_of(t * width, width)
        for c in range(3):
            parts[c, pl.ds(t, 1), :] = xyz[c : c + 1, pl.ds(base, width)]
        return carry

    lax.fori_loop(0, tiles, spread, 0, unroll=8)

    def placed(pairs):
        total = None
        for sel, block in pairs:
            for piece in split3(block):
                term = mm(sel, piece)
                total = term if total is None else total + term
        return total

    total = placed(((first, parts[0]), (second, parts[1])))
    empty = (iota(filled.shape, 0) % 8 < CAP) & (filled < 0.5)
    outgoing[0] = jnp.where(empty, FAR, total).reshape(devices, 8, width)
    others(lambda o, to, where: tile_copy(0, o, to, where).start())
    incoming[0, me] = outgoing[0, me]

    load_rows.wait()
    table = a_buf.reshape(cx * (cy + 2 * PAD), cz)
    column = iota((8, width), 1) - iota((8, width), 0)

    def fetch(t, slot):
        for j in range(width):
            at = rows_s[t, j]
            picked[slot, j // 8, j % 8 : j % 8 + 1, :] = table[pl.ds(at, 1), :]

    def pick(t, slot):
        lanes = jnp.broadcast_to(lanes_v[pl.ds(t, 1), :], (8, width))
        out = jnp.zeros((8, width), F32)
        for m in range(width // 8):
            got = jnp.take_along_axis(picked[slot, m], lanes, axis=1)
            out = jnp.where(column == 8 * m, got, out)
        values[pl.ds(t, 1), :] = jnp.sum(out, axis=0, keepdims=True)

    def gather(t, carry):
        pick(t - 1, (t - 1) % 2)
        fetch(t, t % 2)
        return carry

    early = tiles * EARLY // 64
    fetch(0, 0)
    lax.fori_loop(1, early, gather, 0)

    def finish_gather():
        lax.fori_loop(early, tiles, gather, 0)
        pick(tiles - 1, (tiles - 1) % 2)
        load_coef.wait()
        total = placed(((first, parts[2]), (second, values[...] * coef[...])))
        outgoing[1] = total.reshape(devices, 8, width)
        others(lambda o, to, where: tile_copy(1, o, to, where).start())
        incoming[1, me] = outgoing[1, me]

    load_s.wait()

    def sweep(it, cur, nxt):
        last = it == ITERS - 1
        for c in started[it]:
            c.wait_recv()
        if 0 < it < ITERS - 1:
            for c in started[it - 1][:2]:
                c.wait_send()

        def rows(x, carry):
            cur[x, pl.ds(PAD - 1, 1), :] = hy[it, 0, pl.ds(x, 1), :]
            cur[x, pl.ds(PAD + cy, 1), :] = hy[it, 1, pl.ds(x, 1), :]
            return carry

        lax.fori_loop(0, cx, rows, 0, unroll=8)
        if nfz > 2:
            hz[it, 0] = jnp.where(even, hz[it, 0], hz[it, 1])

        def plane(x, half, below, mid, above, edges):
            y0 = pl.multiple_of(half * band, band)
            span = pl.ds(y0, band)
            edge = pltpu.roll(edges, (2 * cz - 2 * x) - half * (2 * cx), 1)
            total = zsum[x, span, :] + jnp.where(ends, edge, 0.0)
            total = total + cur[x, pl.ds(y0 + (PAD - 1), band), :]
            total = total + cur[x, pl.ds(y0 + (PAD + 1), band), :]
            new = (total + below + above + src[x, span, :]) * inv[x, span, :]
            if last:
                new_p[x, span, :] = new
            else:
                nxt[x, pl.ds(y0 + PAD, band), :] = new

        def at(x, half):
            return cur[x, pl.ds(pl.multiple_of(half * band, band) + PAD, band), :]

        def outer(half, carry):
            span = pl.ds(pl.multiple_of(half * band, band), band)
            edges = hz[it, 0]
            plane(0, half, hx[it, 0, span, :], at(0, half), at(1, half), edges)
            plane(cx - 1, half, at(cx - 2, half), at(cx - 1, half), hx[it, 1, span, :], edges)
            return carry

        for half in range(halves):
            outer(half, 0)
        if not last:
            started.append(x_copies(it + 1, nxt))
            start_x(started[-1])

        def inner(half, carry):
            edges = hz[it, 0]
            below, mid = at(0, half), at(1, half)
            for x in range(1, cx - 1):
                above = at(x + 1, half)
                plane(x, half, below, mid, above, edges)
                below, mid = mid, above
            return carry

        lax.fori_loop(0, halves, inner, 0)
        if not last:
            more = yz_copies(it + 1)
            send_rows(it + 1, nxt)
            for c in more[1:3]:
                c.start()
            pack(it + 1, nxt)
            for c in more[:1] + more[3:]:
                c.start()
            started[-1] = started[-1] + more
            third(nxt)

    slots = devices * CAP
    lines = devices * 8

    def prepare():
        for half in range(2):
            others(lambda o, to, where: tile_copy(half, o, to, where).wait_recv())
        load_lists.wait()
        low = incoming[0].reshape(lines, width)
        high = incoming[1].reshape(lines, width)
        row = iota((lines, slots), 0)
        col = iota((lines, slots), 1)
        home = (row // 8) * CAP + row % CAP
        lower = row % 8 < CAP
        take = (ones_where((home == col) & lower), ones_where((home == col) & (row % 8 >= CAP)))
        for half, block in ((0, low), (1, high)):
            turned = block.T
            for odd in range(2):
                c = 2 * half + odd
                scaled = turned if c == 3 else turned * SCALE
                hi, lo = split2(scaled)
                span = pl.ds(c * width, width)
                tab[span, 0:slots] = mm(hi, take[odd]).astype(BF16)
                tab[span, slots : 2 * slots] = mm(lo, take[odd]).astype(BF16)
        here = ones_where(low < 0.5 * FAR)
        row = iota((slots, lines), 0)
        col = iota((slots, lines), 1)
        home = (col // 8) * CAP + col % CAP
        lower = col % 8 < CAP
        prefix = mm(ones_where((home <= row) & lower), here)
        there = mm(ones_where((home == row) & lower), here)
        place = jnp.where(there > 0.5, prefix - 1.0, -1.0)
        pos[:, 0:width] = place
        pos[:, width : 2 * width] = place
        count = prefix[slots - 1 : slots, 0:1]
        entry = lists[...].astype(F32)
        rest = entry - jnp.floor(entry / count) * count
        rest = jnp.where(rest < 0.0, rest + count, rest)
        want[...] = jnp.where(rest >= count, rest - count, rest)
        load_nodes.wait()

    neigh = lists.shape[0]

    def gauss(block, carry):
        span = pl.ds(pl.multiple_of(block * NODE_BLOCK, NODE_BLOCK), NODE_BLOCK)
        here = [nodes[c : c + 1, span] * SCALE for c in range(3)]
        total = jnp.zeros((8, NODE_BLOCK), F32)
        for k in range(neigh):
            hot = ones_where(pos[...] == want[k : k + 1, span])
            hot = jnp.concatenate([hot, hot], axis=0)
            got = mm(tab[...], hot)
            far = None
            for c in range(3):
                gap = got[c * width : (c + 1) * width] - here[c]
                far = gap * gap if far is None else far + gap * gap
            term = jnp.exp2(-far) * got[3 * width : 4 * width]
            total = total + jnp.sum(term.reshape(width // 8, 8, NODE_BLOCK), axis=0)
        done = jnp.sum(total, axis=0, keepdims=True)
        for h in range(NODE_BLOCK // 128):
            loads[pl.ds(block * (NODE_BLOCK // 128) + h, 1), :] = done[:, h * 128 : (h + 1) * 128]
        return carry

    bufs = (a_buf, b_buf)
    for it in range(ITERS):
        if it == ITERS - 1:
            for group in started[:-1]:
                for c in group[2:]:
                    c.wait_send()
            for c in started[-2][:2] + started[-1]:
                c.wait_send()
            for half in range(2):
                others(lambda o, to, where: tile_copy(half, o, to, where).wait_send())
        sweep(it, bufs[it % 2], bufs[(it + 1) % 2])
        if it == 0:
            finish_gather()
        if it == 1:
            prepare()
        if it < ITERS - 1:
            lax.fori_loop(gauss_bounds[it], gauss_bounds[it + 1], gauss, 0)


def on_device(
    sizes,
    pressure, source, diag_shift, iface_cells, iface_coef, iface_xyz, node_xyz, owners, node_lists,
):
    nfx, nfy, nfz = sizes
    devices = nfx * nfy * nfz
    tiles = owners.shape[0]
    width = iface_coef.shape[0] // tiles
    cx, cy, cz = pressure.shape
    nodes, neigh = node_lists.shape
    vmem = pl.BlockSpec(memory_space=pltpu.VMEM)
    hbm = pl.BlockSpec(memory_space=pltpu.HBM)
    slots = devices * CAP
    blocks = nodes // NODE_BLOCK
    bounds = [0, 0] + [blocks * i // (ITERS - 2) for i in range(1, ITERS - 1)]
    dma = pltpu.SemaphoreType.DMA

    def space(*shape, dtype=F32):
        return pltpu.VMEM(shape, dtype)

    new_p, loads = pl.pallas_call(
        functools.partial(main_kernel, sizes, bounds),
        out_shape=(
            jax.ShapeDtypeStruct((cx, cy, cz), F32),
            jax.ShapeDtypeStruct((nodes // 128, 128), F32),
        ),
        in_specs=[hbm] * 9,
        out_specs=(vmem, vmem),
        scratch_shapes=[
            space(cx, cy + 2 * PAD, cz),
            space(cx, cy + 2 * PAD, cz),
            space(cx, cy, cz),
            space(cx, cy, cz),
            space(cx, cy, cz),
            space(ITERS, 2, cy, cz),
            space(ITERS, 2, cx, cz),
            space(ITERS, 2, 2 * cx * cy // cz, cz),
            space(ITERS, 2, cx, cz),
            space(ITERS, 2 * cx * cy // cz, cz),
            space(2 * cz, cz, dtype=BF16),
            space(tiles, width, dtype=jnp.int32),
            space(tiles, width, dtype=jnp.int32),
            space(tiles, width, dtype=jnp.int32),
            pltpu.SMEM((tiles, width), jnp.int32),
            space(tiles, width),
            space(3, tiles * width),
            space(1, tiles, dtype=jnp.int32),
            space(3, nodes),
            space(neigh, nodes, dtype=jnp.int32),
            space(2, width // 8, 8, width),
            space(3, tiles, width),
            space(tiles, width),
            space(2, devices, 8, width),
            space(2, devices, 8, width),
            space(4 * width, 2 * slots, dtype=BF16),
            space(slots, NODE_BLOCK),
            space(neigh, nodes),
            dma((9,)),
            dma((ITERS, 2)), dma((ITERS, 2)),
            dma((ITERS, 2)), dma((ITERS, 2)),
            dma((ITERS, 2)), dma((ITERS, 2)),
            dma((2, devices)), dma((2, devices)),
        ],
        compiler_params=pltpu.CompilerParams(
            collective_id=0, has_side_effects=True, vmem_limit_bytes=56 * 1024 * 1024
        ),
        name="sweeps",
    )(
        pressure,
        source,
        diag_shift,
        iface_cells.reshape(tiles, width),
        iface_coef.reshape(tiles, width),
        iface_xyz,
        owners.reshape(1, tiles),
        node_xyz,
        node_lists.T,
    )
    return new_p, loads.reshape(nodes)


def solution(mesh):
    sizes = tuple(mesh.shape[a] for a in ("fx", "fy", "fz"))
    cells = P("fx", "fy", "fz")
    flat = P(("fx", "fy", "fz"))
    return jax.shard_map(
        functools.partial(on_device, sizes),
        mesh=mesh,
        in_specs=(
            cells, cells, cells, flat, flat,
            P(None, ("fx", "fy", "fz")), P(None, ("fx", "fy", "fz")), flat,
            P(("fx", "fy", "fz"), None),
        ),
        out_specs=(cells, flat),
        check_vma=False,
    )
```

```python
import functools
import math

import jax
import jax.numpy as jnp
from jax import lax
from jax.experimental import pallas as pl
from jax.experimental.pallas import tpu as pltpu
from jax.sharding import PartitionSpec as P

ITERS = 4
CAP = 4
GAUSS_RATE = 0.5
SCALE = math.sqrt(GAUSS_RATE * math.log2(math.e))
FAR = 1.0e6
NODE_BLOCK = 256
PAD = 8
MESH = pl.DeviceIdType.MESH
F32 = jnp.float32
BF16 = jnp.bfloat16
EARLY = 24


def split2(x):
    hi = x.astype(BF16)
    return hi, (x - hi.astype(F32)).astype(BF16)


def split3(x):
    hi = x.astype(BF16)
    rest = x - hi.astype(F32)
    mid = rest.astype(BF16)
    return hi, mid, (rest - mid.astype(F32)).astype(BF16)


def mm(a, b):
    return jnp.dot(a, b, preferred_element_type=F32)


def iota(shape, dim):
    return lax.broadcasted_iota(jnp.int32, shape, dim)


def ones_where(mask):
    return jnp.where(mask, 1.0, 0.0).astype(BF16)


def main_kernel(
    sizes, gauss_bounds,
    p_any, s_any, d_any, cells_any, coef_any, xyz_any, own_any, nodes_any, lists_any,
    new_p, loads,
    a_buf, b_buf, src, inv, zsum, hx, hy, hz, ys, zs, shift,
    cells, lanes_v, rows_v, rows_s, coef, xyz, own_v, nodes, lists,
    picked, parts, values, outgoing, incoming, tab, pos, want,
    word_sem, load_sem, x_send, x_recv, y_send, y_recv, z_send, z_recv, t_send, t_recv,
):
    nfx, nfy, nfz = sizes
    devices = nfx * nfy * nfz
    cx, cy, cz = src.shape
    tiles, width = coef.shape
    bx, by, bz = lax.axis_index("fx"), lax.axis_index("fy"), lax.axis_index("fz")
    me = (bx * nfy + by) * nfz + bz
    body = pl.ds(PAD, cy)

    def local(a, b, k):
        return pltpu.make_async_copy(a, b, load_sem.at[k])

    tx = [(bx + d) % nfx for d in range(nfx)]
    ty = [(by + d) % nfy for d in range(nfy)]
    tz = [(bz + d) % nfz for d in range(nfz)]
    x_next, x_prev = (tx[1 % nfx], by, bz), (tx[nfx - 1], by, bz)
    y_next, y_prev = (bx, ty[1 % nfy], bz), (bx, ty[nfy - 1], bz)
    z_next, z_prev = (bx, by, tz[1 % nfz]), (bx, by, tz[nfz - 1])
    beside = [
        [there] if count == 2 else [there, back]
        for count, there, back in (
            (nfx, x_next, x_prev), (nfy, y_next, y_prev), (nfz, z_next, z_prev)
        )
    ]

    def signal(sem, device):
        pl.semaphore_signal(sem, inc=1, device_id=device, device_id_type=MESH)

    barrier = pltpu.get_barrier_semaphore()
    for group in beside:
        for device in group:
            signal(barrier, device)

    words = [beside[0]] * (nfx // 2 - 1) + [beside[1]] * (nfy // 2) + [beside[2]] * (nfz // 2)
    spread_to = [0]

    def pass_word():
        k = spread_to[0]
        if 0 < k <= len(words):
            pl.semaphore_wait(word_sem.at[k - 1], len(words[k - 1]))
        if k < len(words):
            for device in words[k]:
                signal(word_sem.at[k], device)
        spread_to[0] = k + 1

    inside = pl.ds(1, cx - 2)
    load_low = local(p_any.at[0], a_buf.at[0, body], 0)
    load_high = local(p_any.at[cx - 1], a_buf.at[cx - 1, body], 1)
    load_p = local(p_any.at[inside], a_buf.at[inside, body, :], 2)
    load_cells = local(cells_any, cells, 3)
    load_own = local(own_any, own_v, 4)
    load_xyz = local(xyz_any, xyz, 5)
    load_d = local(d_any, inv, 6)
    load_s = local(s_any, src, 7)
    load_coef = local(coef_any, coef, 8)
    load_nodes = local(nodes_any, nodes, 9)
    load_lists = local(lists_any, lists, 10)
    for c in (
        load_low, load_high, load_p, load_cells, load_own, load_xyz,
        load_d, load_s, load_coef, load_nodes, load_lists,
    ):
        c.start()

    def others(act):
        def inner(x_to, first, base):
            for dy in range(nfy):
                for dz in range(nfz):
                    if first and dy == 0 and dz == 0:
                        continue
                    to = (x_to * nfy + ty[dy]) * nfz + tz[dz]
                    act(base + dy * nfz + dz, to, (x_to, ty[dy], tz[dz]))

        inner(tx[0], True, 0)

        def step(d, carry):
            inner((bx + d) % nfx, False, d * (nfy * nfz))
            return carry

        lax.fori_loop(1, nfx, step, 0)

    def remote(a, b, ss, rs, device):
        return pltpu.make_async_remote_copy(
            src_ref=a, dst_ref=b, send_sem=ss, recv_sem=rs, device_id=device, device_id_type=MESH
        )

    def tile_copy(half, o, to, where):
        return remote(
            outgoing.at[half, to], incoming.at[half, me],
            t_send.at[half, o], t_recv.at[half, o], where,
        )

    def x_copies(it, buf):
        return [
            remote(buf.at[cx - 1, body], hx.at[it, 0], x_send.at[it, 0], x_recv.at[it, 0], x_next),
            remote(buf.at[0, body], hx.at[it, 1], x_send.at[it, 1], x_recv.at[it, 1], x_prev),
        ]

    def start_x(copies):
        @pl.when(bx == 0)
        def _():
            copies[1].start()
            copies[0].start()

        @pl.when(bx != 0)
        def _():
            copies[0].start()
            copies[1].start()

    def yz_copies(it):
        made = [
            remote(zs.at[it], hz.at[it, 0], z_send.at[it, 0], z_recv.at[it, 0], z_next),
            remote(ys.at[it, 1], hy.at[it, 0], y_send.at[it, 0], y_recv.at[it, 0], y_next),
            remote(ys.at[it, 0], hy.at[it, 1], y_send.at[it, 1], y_recv.at[it, 1], y_prev),
        ]
        if nfz > 2:
            made.append(
                remote(zs.at[it], hz.at[it, 1], z_send.at[it, 1], z_recv.at[it, 1], z_prev)
            )
        return made

    halves = cz // (2 * cx)
    band = cy // halves
    lane = iota((band, cz), 1)
    pair = lax.shift_right_logical(lane, 1)
    even = lane % 2 == 0
    ends = (lane == 0) | (lane == cz - 1)

    def send_rows(it, buf):
        def one(x, carry):
            ys[it, 0, pl.ds(x, 1), :] = buf[x, pl.ds(PAD, 1), :]
            ys[it, 1, pl.ds(x, 1), :] = buf[x, pl.ds(PAD + cy - 1, 1), :]
            return carry

        lax.fori_loop(0, cx, one, 0, unroll=8)

    def pack_only(half, buf, packed):
        y0 = pl.multiple_of(half * band, band)
        for x in range(cx):
            moved = pltpu.roll(buf[x, pl.ds(y0 + PAD, band), :], half * (2 * cx) + (2 * x + 1), 1)
            packed = jnp.where(pair == x + half * cx, moved, packed)
        return packed

    def third_only(half, buf):
        y0 = pl.multiple_of(half * band, band)
        hi, lo = split2(buf[:, pl.ds(y0 + PAD, band), :].reshape(cx * band, cz))
        near = mm(jnp.concatenate([hi, lo], axis=1), shift[...])
        zsum[:, pl.ds(y0, band), :] = near.reshape(cx, band, cz)

    def store_packed(it, packed):
        zs[it] = jnp.where(even, packed, pltpu.roll(packed, cz - 2, 1))

    def pack(it, buf):
        packed = jnp.zeros((band, cz), F32)
        packed = lax.fori_loop(0, halves, lambda half, z: pack_only(half, buf, z), packed)
        store_packed(it, packed)

    def third(buf):
        lax.fori_loop(0, halves, lambda half, z: (third_only(half, buf), z)[1], 0)

    def pack_third(it, buf):
        def both(half, packed):
            third_only(half, buf)
            return pack_only(half, buf, packed)

        store_packed(it, lax.fori_loop(0, halves, both, jnp.zeros((band, cz), F32)))

    apart = jnp.abs(iota((cz, cz), 0) - iota((cz, cz), 1))
    for part in range(2):
        shift[part * cz : (part + 1) * cz, :] = ones_where(apart == 1)

    load_low.wait()
    load_high.wait()
    pl.semaphore_wait(barrier, sum(len(group) for group in beside))
    started = [x_copies(0, a_buf)]
    start_x(started[0])
    started[0] = started[0] + yz_copies(0)
    pass_word()
    load_p.wait()
    send_rows(0, a_buf)
    for c in started[0][3:5]:
        c.start()
    pack(0, a_buf)
    for c in started[0][2:3] + started[0][5:]:
        c.start()
    pass_word()

    third(a_buf)
    pass_word()
    load_d.wait()

    def invert(x, carry):
        inv[x] = 1.0 / (6.0 + inv[x])
        return carry

    lax.fori_loop(0, cx, invert, 0, unroll=4)

    load_cells.wait()
    flat = cells[...]
    row_of = lax.shift_right_logical(flat, cz.bit_length() - 1)
    plane_of = lax.shift_right_logical(row_of, cy.bit_length() - 1)
    rows_v[...] = row_of + plane_of * (2 * PAD) + PAD
    lanes_v[...] = jnp.bitwise_and(flat, cz - 1)

    load_rows = pltpu.make_async_copy(rows_v, rows_s, load_sem.at[3])
    load_rows.start()
    pass_word()

    load_own.wait()
    own = own_v[...]
    mine = iota((devices, tiles), 0) == own
    before = ones_where(iota((tiles, tiles), 0) < iota((tiles, tiles), 1))
    earlier = mm(ones_where(mine), before)
    rank = jnp.sum(jnp.where(mine, earlier, 0.0), axis=0, keepdims=True)
    target = own * CAP + rank.astype(jnp.int32)
    line = iota((devices * 8, tiles), 0)
    at_slot = (line // 8) * CAP + line % CAP == target
    low_rows = line % 8 < CAP
    first = ones_where(at_slot & low_rows)
    second = ones_where(at_slot & jnp.logical_not(low_rows))
    filled = mm(first, jnp.ones((tiles, width), BF16))

    load_xyz.wait()

    def spread(t, carry):
        base = pl.multiple_of(t * width, width)
        for c in range(3):
            parts[c, pl.ds(t, 1), :] = xyz[c : c + 1, pl.ds(base, width)]
        return carry

    lax.fori_loop(0, tiles, spread, 0, unroll=8)

    def placed(pairs):
        total = None
        for sel, block in pairs:
            for piece in split3(block):
                term = mm(sel, piece)
                total = term if total is None else total + term
        return total

    pass_word()
    total = placed(((first, parts[0]), (second, parts[1])))
    empty = (iota(filled.shape, 0) % 8 < CAP) & (filled < 0.5)
    outgoing[0] = jnp.where(empty, FAR, total).reshape(devices, 8, width)
    while spread_to[0] <= len(words):
        pass_word()
    others(lambda o, to, where: tile_copy(0, o, to, where).start())
    incoming[0, me] = outgoing[0, me]

    load_rows.wait()
    table = a_buf.reshape(cx * (cy + 2 * PAD), cz)
    column = iota((8, width), 1) - iota((8, width), 0)

    def fetch(t, slot):
        places = rows_s.at[t]
        for j in range(width):
            at = places[j]
            picked[slot, j // 8, j % 8 : j % 8 + 1, :] = table[pl.ds(at, 1), :]

    def pick(t, slot):
        lanes = jnp.broadcast_to(lanes_v[pl.ds(t, 1), :], (8, width))
        out = jnp.zeros((8, width), F32)
        for m in range(width // 8):
            got = jnp.take_along_axis(picked[slot, m], lanes, axis=1)
            out = jnp.where(column == 8 * m, got, out)
        values[pl.ds(t, 1), :] = jnp.sum(out, axis=0, keepdims=True)

    def gather(t, carry):
        pick(t - 1, (t - 1) % 2)
        fetch(t, t % 2)
        return carry

    fetch(0, 0)
    early = tiles * EARLY // 64
    lax.fori_loop(1, early, gather, 0)

    def finish_gather():
        lax.fori_loop(early, tiles, gather, 0)
        pick(tiles - 1, (tiles - 1) % 2)
        load_coef.wait()
        total = placed(((first, parts[2]), (second, values[...] * coef[...])))
        outgoing[1] = total.reshape(devices, 8, width)
        others(lambda o, to, where: tile_copy(1, o, to, where).start())
        incoming[1, me] = outgoing[1, me]

    load_s.wait()

    save_edges = [
        local(zsum.at[0], new_p.at[0], 11),
        local(zsum.at[cx - 1], new_p.at[cx - 1], 12),
    ]
    saves = list(save_edges)

    def sweep(it, cur, nxt):
        last = it == ITERS - 1
        for c in started[it]:
            c.wait_recv()
        if 0 < it < ITERS - 1:
            for c in started[it - 1][:2]:
                c.wait_send()

        def rows(x, carry):
            cur[x, pl.ds(PAD - 1, 1), :] = hy[it, 0, pl.ds(x, 1), :]
            cur[x, pl.ds(PAD + cy, 1), :] = hy[it, 1, pl.ds(x, 1), :]
            return carry

        lax.fori_loop(0, cx, rows, 0, unroll=8)
        if nfz > 2:
            hz[it, 0] = jnp.where(even, hz[it, 0], hz[it, 1])

        def plane(x, half, below, mid, above, edges):
            y0 = pl.multiple_of(half * band, band)
            span = pl.ds(y0, band)
            edge = pltpu.roll(edges, (2 * cz - 2 * x) - half * (2 * cx), 1)
            total = zsum[x, span, :] + jnp.where(ends, edge, 0.0)
            total = total + cur[x, pl.ds(y0 + (PAD - 1), band), :]
            total = total + cur[x, pl.ds(y0 + (PAD + 1), band), :]
            new = (total + below + above + src[x, span, :]) * inv[x, span, :]
            if last:
                zsum[x, span, :] = new
            else:
                nxt[x, pl.ds(y0 + PAD, band), :] = new

        def at(x, half):
            return cur[x, pl.ds(pl.multiple_of(half * band, band) + PAD, band), :]

        def outer(half, carry):
            span = pl.ds(pl.multiple_of(half * band, band), band)
            edges = hz[it, 0]
            plane(0, half, hx[it, 0, span, :], at(0, half), at(1, half), edges)
            plane(cx - 1, half, at(cx - 2, half), at(cx - 1, half), hx[it, 1, span, :], edges)
            return carry

        for half in range(halves):
            outer(half, 0)
        if last:
            save_edges[0].start()
            save_edges[1].start()
        if not last:
            started.append(x_copies(it + 1, nxt))
            start_x(started[-1])

        def inner(half, carry):
            edges = hz[it, 0]
            below, mid = at(0, half), at(1, half)
            for x in range(1, cx - 1):
                above = at(x + 1, half)
                plane(x, half, below, mid, above, edges)
                below, mid = mid, above
            return carry

        if last:
            for half in range(halves):
                inner(half, 0)
                rows_of = pl.ds(half * band, band)
                save = local(zsum.at[inside, rows_of], new_p.at[inside, rows_of], half)
                save.start()
                saves.append(save)
        else:
            lax.fori_loop(0, halves, inner, 0)
            more = yz_copies(it + 1)
            send_rows(it + 1, nxt)
            for c in more[1:3]:
                c.start()
            pack_third(it + 1, nxt)
            for c in more[:1] + more[3:]:
                c.start()
            started[-1] = started[-1] + more

    slots = devices * CAP
    lines = devices * 8

    def prepare():
        for half in range(2):
            others(lambda o, to, where: tile_copy(half, o, to, where).wait_recv())
        load_lists.wait()
        low = incoming[0].reshape(lines, width)
        high = incoming[1].reshape(lines, width)
        row = iota((lines, slots), 0)
        col = iota((lines, slots), 1)
        home = (row // 8) * CAP + row % CAP
        lower = row % 8 < CAP
        take = (ones_where((home == col) & lower), ones_where((home == col) & (row % 8 >= CAP)))
        for half, block in ((0, low), (1, high)):
            turned = block.T
            for odd in range(2):
                c = 2 * half + odd
                scaled = turned if c == 3 else turned * SCALE
                hi, lo = split2(scaled)
                span = pl.ds(c * width, width)
                tab[span, 0:slots] = mm(hi, take[odd]).astype(BF16)
                tab[span, slots : 2 * slots] = mm(lo, take[odd]).astype(BF16)
        here = ones_where(low < 0.5 * FAR)
        row = iota((slots, lines), 0)
        col = iota((slots, lines), 1)
        home = (col // 8) * CAP + col % CAP
        lower = col % 8 < CAP
        prefix = mm(ones_where((home <= row) & lower), here)
        there = mm(ones_where((home == row) & lower), here)
        place = jnp.where(there > 0.5, prefix - 1.0, -1.0)
        pos[:, 0:width] = place
        pos[:, width : 2 * width] = place
        count = prefix[slots - 1 : slots, 0:1]
        entry = lists[...].astype(F32)
        rest = entry - jnp.floor(entry / count) * count
        rest = jnp.where(rest < 0.0, rest + count, rest)
        want[...] = jnp.where(rest >= count, rest - count, rest)
        load_nodes.wait()

    neigh = lists.shape[0]

    def gauss(block, carry):
        span = pl.ds(pl.multiple_of(block * NODE_BLOCK, NODE_BLOCK), NODE_BLOCK)
        here = [nodes[c : c + 1, span] * SCALE for c in range(3)]
        total = jnp.zeros((8, NODE_BLOCK), F32)
        for k in range(neigh):
            hot = ones_where(pos[...] == want[k : k + 1, span])
            hot = jnp.concatenate([hot, hot], axis=0)
            got = mm(tab[...], hot)
            far = None
            for c in range(3):
                gap = got[c * width : (c + 1) * width] - here[c]
                far = gap * gap if far is None else far + gap * gap
            term = jnp.exp2(-far) * got[3 * width : 4 * width]
            total = total + jnp.sum(term.reshape(width // 8, 8, NODE_BLOCK), axis=0)
        done = jnp.sum(total, axis=0, keepdims=True)
        for h in range(NODE_BLOCK // 128):
            loads[pl.ds(block * (NODE_BLOCK // 128) + h, 1), :] = done[:, h * 128 : (h + 1) * 128]
        return carry

    bufs = (a_buf, b_buf)
    for it in range(ITERS):
        if it == ITERS - 1:
            for group in started[:-1]:
                for c in group[2:]:
                    c.wait_send()
            for c in started[-2][:2] + started[-1]:
                c.wait_send()
            for half in range(2):
                others(lambda o, to, where: tile_copy(half, o, to, where).wait_send())
        sweep(it, bufs[it % 2], bufs[(it + 1) % 2])
        if it == 0:
            finish_gather()
        if it == 1:
            prepare()
        if it < ITERS - 1:
            lax.fori_loop(gauss_bounds[it], gauss_bounds[it + 1], gauss, 0)
    for c in saves:
        c.wait()


def copy_kernel(parts, p_any, loads_any, p_out, loads_out, held, held_loads, sem_in, sem_out):
    depth = p_any.shape[0] // parts
    moves = []
    for i in range(parts):
        span = pl.ds(i * depth, depth)
        moves.append(
            (
                pltpu.make_async_copy(p_any.at[span], held.at[span], sem_in.at[i]),
                pltpu.make_async_copy(held.at[span], p_out.at[span], sem_out.at[i]),
            )
        )
    moves.append(
        (
            pltpu.make_async_copy(loads_any, held_loads, sem_in.at[parts]),
            pltpu.make_async_copy(held_loads, loads_out, sem_out.at[parts]),
        )
    )
    for into, _ in moves:
        into.start()
    for into, out in moves:
        into.wait()
        out.start()
    for _, out in moves:
        out.wait()


def on_device(
    sizes,
    pressure, source, diag_shift, iface_cells, iface_coef, iface_xyz, node_xyz, owners, node_lists,
):
    nfx, nfy, nfz = sizes
    devices = nfx * nfy * nfz
    tiles = owners.shape[0]
    width = iface_coef.shape[0] // tiles
    cx, cy, cz = pressure.shape
    nodes, neigh = node_lists.shape
    vmem = pl.BlockSpec(memory_space=pltpu.VMEM)
    hbm = pl.BlockSpec(memory_space=pltpu.HBM)
    slots = devices * CAP
    blocks = nodes // NODE_BLOCK
    bounds = [blocks * i // 8 for i in (0, 0, 2, 8)]
    dma = pltpu.SemaphoreType.DMA

    def space(*shape, dtype=F32):
        return pltpu.VMEM(shape, dtype)

    new_p, loads = pl.pallas_call(
        functools.partial(main_kernel, sizes, bounds),
        out_shape=(
            jax.ShapeDtypeStruct((cx, cy, cz), F32),
            jax.ShapeDtypeStruct((nodes // 128, 128), F32),
        ),
        in_specs=[hbm] * 9,
        out_specs=(hbm, vmem),
        scratch_shapes=[
            space(cx, cy + 2 * PAD, cz),
            space(cx, cy + 2 * PAD, cz),
            space(cx, cy, cz),
            space(cx, cy, cz),
            space(cx, cy, cz),
            space(ITERS, 2, cy, cz),
            space(ITERS, 2, cx, cz),
            space(ITERS, 2, 2 * cx * cy // cz, cz),
            space(ITERS, 2, cx, cz),
            space(ITERS, 2 * cx * cy // cz, cz),
            space(2 * cz, cz, dtype=BF16),
            space(tiles, width, dtype=jnp.int32),
            space(tiles, width, dtype=jnp.int32),
            space(tiles, width, dtype=jnp.int32),
            pltpu.SMEM((tiles, width), jnp.int32),
            space(tiles, width),
            space(3, tiles * width),
            space(1, tiles, dtype=jnp.int32),
            space(3, nodes),
            space(neigh, nodes, dtype=jnp.int32),
            space(2, width // 8, 8, width),
            space(3, tiles, width),
            space(tiles, width),
            space(2, devices, 8, width),
            space(2, devices, 8, width),
            space(4 * width, 2 * slots, dtype=BF16),
            space(slots, NODE_BLOCK),
            space(neigh, nodes),
            pltpu.SemaphoreType.REGULAR((nfx // 2 + nfy // 2 + nfz // 2,)),
            dma((13,)),
            dma((ITERS, 2)), dma((ITERS, 2)),
            dma((ITERS, 2)), dma((ITERS, 2)),
            dma((ITERS, 2)), dma((ITERS, 2)),
            dma((2, devices)), dma((2, devices)),
        ],
        compiler_params=pltpu.CompilerParams(
            collective_id=0, has_side_effects=True, vmem_limit_bytes=56 * 1024 * 1024
        ),
        name="sweeps",
    )(
        pressure,
        source,
        diag_shift,
        iface_cells.reshape(tiles, width),
        iface_coef.reshape(tiles, width),
        iface_xyz,
        owners.reshape(1, tiles),
        node_xyz,
        node_lists.T,
    )
    pieces = 4
    new_p, loads = pl.pallas_call(
        functools.partial(copy_kernel, pieces),
        out_shape=(
            jax.ShapeDtypeStruct((cx, cy, cz), F32),
            jax.ShapeDtypeStruct((nodes // 128, 128), F32),
        ),
        in_specs=[hbm, hbm],
        out_specs=(hbm, hbm),
        scratch_shapes=[
            space(cx, cy, cz),
            space(nodes // 128, 128),
            dma((pieces + 1,)),
            dma((pieces + 1,)),
        ],
        compiler_params=pltpu.CompilerParams(vmem_limit_bytes=56 * 1024 * 1024),
        name="place",
    )(new_p, loads)
    return new_p, loads.reshape(nodes)


def solution(mesh):
    sizes = tuple(mesh.shape[a] for a in ("fx", "fy", "fz"))
    cells = P("fx", "fy", "fz")
    flat = P(("fx", "fy", "fz"))
    return jax.shard_map(
        functools.partial(on_device, sizes),
        mesh=mesh,
        in_specs=(
            cells, cells, cells, flat, flat,
            P(None, ("fx", "fy", "fz")), P(None, ("fx", "fy", "fz")), flat,
            P(("fx", "fy", "fz"), None),
        ),
        out_specs=(cells, flat),
        check_vma=False,
    )
```

```python
import functools
import math

import jax
import jax.numpy as jnp
from jax import lax
from jax.experimental import pallas as pl
from jax.experimental.pallas import tpu as pltpu
from jax.sharding import PartitionSpec as P

ITERS = 4
CAP = 4
GAUSS_RATE = 0.5
SCALE = math.sqrt(GAUSS_RATE * math.log2(math.e))
FAR = 1.0e6
NODE_BLOCK = 256
PAD = 8
MESH = pl.DeviceIdType.MESH
F32 = jnp.float32
BF16 = jnp.bfloat16
EARLY = 28


def split2(x):
    hi = x.astype(BF16)
    return hi, (x - hi.astype(F32)).astype(BF16)


def split3(x):
    hi = x.astype(BF16)
    rest = x - hi.astype(F32)
    mid = rest.astype(BF16)
    return hi, mid, (rest - mid.astype(F32)).astype(BF16)


def mm(a, b):
    return jnp.dot(a, b, preferred_element_type=F32)


def iota(shape, dim):
    return lax.broadcasted_iota(jnp.int32, shape, dim)


def ones_where(mask):
    return jnp.where(mask, 1.0, 0.0).astype(BF16)


def main_kernel(
    sizes, gauss_bounds,
    p_any, s_any, d_any, cells_any, coef_any, xyz_any, own_any, nodes_any, lists_any,
    new_p, loads,
    a_buf, b_buf, src, inv, zsum, hx, hy, hz, ys, zs, shift,
    cells, lanes_v, rows_v, rows_s, coef, xyz, own_v, nodes, lists,
    picked, parts, values, outgoing, incoming, tab, pos, want,
    load_sem, x_send, x_recv, y_send, y_recv, z_send, z_recv, t_send, t_recv,
):
    nfx, nfy, nfz = sizes
    devices = nfx * nfy * nfz
    cx, cy, cz = src.shape
    tiles, width = coef.shape
    bx, by, bz = lax.axis_index("fx"), lax.axis_index("fy"), lax.axis_index("fz")
    me = (bx * nfy + by) * nfz + bz
    body = pl.ds(PAD, cy)

    def local(a, b, k):
        return pltpu.make_async_copy(a, b, load_sem.at[k])

    tx = [(bx + d) % nfx for d in range(nfx)]
    ty = [(by + d) % nfy for d in range(nfy)]
    tz = [(bz + d) % nfz for d in range(nfz)]
    x_next, x_prev = (tx[1 % nfx], by, bz), (tx[nfx - 1], by, bz)
    y_next, y_prev = (bx, ty[1 % nfy], bz), (bx, ty[nfy - 1], bz)
    z_next, z_prev = (bx, by, tz[1 % nfz]), (bx, by, tz[nfz - 1])
    inside = pl.ds(1, cx - 2)
    load_low = local(p_any.at[0], a_buf.at[0, body], 0)
    load_high = local(p_any.at[cx - 1], a_buf.at[cx - 1, body], 1)
    load_p = local(p_any.at[inside], a_buf.at[inside, body, :], 2)
    load_cells = local(cells_any, cells, 3)
    load_own = local(own_any, own_v, 4)
    load_xyz = local(xyz_any, xyz, 5)
    load_d = local(d_any, inv, 6)
    load_s = local(s_any, src, 7)
    load_coef = local(coef_any, coef, 8)
    load_nodes = local(nodes_any, nodes, 9)
    load_lists = local(lists_any, lists, 10)
    for c in (
        load_low, load_high, load_p, load_cells, load_own, load_xyz,
        load_d, load_s, load_coef, load_nodes, load_lists,
    ):
        c.start()

    def others(act):
        def inner(x_to, first, base):
            for dy in range(nfy):
                for dz in range(nfz):
                    if first and dy == 0 and dz == 0:
                        continue
                    to = (x_to * nfy + ty[dy]) * nfz + tz[dz]
                    act(base + dy * nfz + dz, to, (x_to, ty[dy], tz[dz]))

        inner(tx[0], True, 0)

        def step(d, carry):
            inner((bx + d) % nfx, False, d * (nfy * nfz))
            return carry

        lax.fori_loop(1, nfx, step, 0)

    barrier = pltpu.get_barrier_semaphore()
    others(
        lambda o, to, where: pl.semaphore_signal(
            barrier, inc=1, device_id=where, device_id_type=MESH
        )
    )

    def remote(a, b, ss, rs, device):
        return pltpu.make_async_remote_copy(
            src_ref=a, dst_ref=b, send_sem=ss, recv_sem=rs, device_id=device, device_id_type=MESH
        )

    def tile_copy(half, o, to, where):
        return remote(
            outgoing.at[half, to], incoming.at[half, me],
            t_send.at[half, o], t_recv.at[half, o], where,
        )

    def x_copies(it, buf):
        return [
            remote(buf.at[cx - 1, body], hx.at[it, 0], x_send.at[it, 0], x_recv.at[it, 0], x_next),
            remote(buf.at[0, body], hx.at[it, 1], x_send.at[it, 1], x_recv.at[it, 1], x_prev),
        ]

    def start_x(copies):
        @pl.when(bx == 0)
        def _():
            copies[1].start()
            copies[0].start()

        @pl.when(bx != 0)
        def _():
            copies[0].start()
            copies[1].start()

    def yz_copies(it):
        made = [
            remote(zs.at[it], hz.at[it, 0], z_send.at[it, 0], z_recv.at[it, 0], z_next),
            remote(ys.at[it, 1], hy.at[it, 0], y_send.at[it, 0], y_recv.at[it, 0], y_next),
            remote(ys.at[it, 0], hy.at[it, 1], y_send.at[it, 1], y_recv.at[it, 1], y_prev),
        ]
        if nfz > 2:
            made.append(
                remote(zs.at[it], hz.at[it, 1], z_send.at[it, 1], z_recv.at[it, 1], z_prev)
            )
        return made

    halves = cz // (2 * cx)
    band = cy // halves
    lane = iota((band, cz), 1)
    pair = lax.shift_right_logical(lane, 1)
    even = lane % 2 == 0
    ends = (lane == 0) | (lane == cz - 1)

    def send_rows(it, buf):
        def one(x, carry):
            ys[it, 0, pl.ds(x, 1), :] = buf[x, pl.ds(PAD, 1), :]
            ys[it, 1, pl.ds(x, 1), :] = buf[x, pl.ds(PAD + cy - 1, 1), :]
            return carry

        lax.fori_loop(0, cx, one, 0, unroll=8)

    def pack_only(half, buf, packed):
        y0 = pl.multiple_of(half * band, band)
        for x in range(cx):
            moved = pltpu.roll(buf[x, pl.ds(y0 + PAD, band), :], half * (2 * cx) + (2 * x + 1), 1)
            packed = jnp.where(pair == x + half * cx, moved, packed)
        return packed

    def third_only(half, buf):
        y0 = pl.multiple_of(half * band, band)
        hi, lo = split2(buf[:, pl.ds(y0 + PAD, band), :].reshape(cx * band, cz))
        near = mm(jnp.concatenate([hi, lo], axis=1), shift[...])
        zsum[:, pl.ds(y0, band), :] = near.reshape(cx, band, cz)

    def store_packed(it, packed):
        zs[it] = jnp.where(even, packed, pltpu.roll(packed, cz - 2, 1))

    def pack(it, buf):
        packed = jnp.zeros((band, cz), F32)
        packed = lax.fori_loop(0, halves, lambda half, z: pack_only(half, buf, z), packed)
        store_packed(it, packed)

    def third(buf):
        lax.fori_loop(0, halves, lambda half, z: (third_only(half, buf), z)[1], 0)

    def pack_third(it, buf):
        def both(half, packed):
            third_only(half, buf)
            return pack_only(half, buf, packed)

        store_packed(it, lax.fori_loop(0, halves, both, jnp.zeros((band, cz), F32)))

    apart = jnp.abs(iota((cz, cz), 0) - iota((cz, cz), 1))
    for part in range(2):
        shift[part * cz : (part + 1) * cz, :] = ones_where(apart == 1)

    load_low.wait()
    load_high.wait()
    load_p.wait()
    send_rows(0, a_buf)
    pack(0, a_buf)
    load_cells.wait()
    flat = cells[...]
    row_of = lax.shift_right_logical(flat, cz.bit_length() - 1)
    plane_of = lax.shift_right_logical(row_of, cy.bit_length() - 1)
    rows_v[...] = row_of + plane_of * (2 * PAD) + PAD
    lanes_v[...] = jnp.bitwise_and(flat, cz - 1)

    load_rows = pltpu.make_async_copy(rows_v, rows_s, load_sem.at[3])
    load_rows.start()

    load_own.wait()
    own = own_v[...]
    mine = iota((devices, tiles), 0) == own
    before = ones_where(iota((tiles, tiles), 0) < iota((tiles, tiles), 1))
    earlier = mm(ones_where(mine), before)
    rank = jnp.sum(jnp.where(mine, earlier, 0.0), axis=0, keepdims=True)
    target = own * CAP + rank.astype(jnp.int32)
    line = iota((devices * 8, tiles), 0)
    at_slot = (line // 8) * CAP + line % CAP == target
    low_rows = line % 8 < CAP
    first = ones_where(at_slot & low_rows)
    second = ones_where(at_slot & jnp.logical_not(low_rows))
    filled = mm(first, jnp.ones((tiles, width), BF16))

    load_xyz.wait()

    def spread(t, carry):
        base = pl.multiple_of(t * width, width)
        for c in range(3):
            parts[c, pl.ds(t, 1), :] = xyz[c : c + 1, pl.ds(base, width)]
        return carry

    lax.fori_loop(0, tiles, spread, 0, unroll=8)

    def placed(pairs):
        total = None
        for sel, block in pairs:
            for piece in split3(block):
                term = mm(sel, piece)
                total = term if total is None else total + term
        return total

    total = placed(((first, parts[0]), (second, parts[1])))
    empty = (iota(filled.shape, 0) % 8 < CAP) & (filled < 0.5)
    outgoing[0] = jnp.where(empty, FAR, total).reshape(devices, 8, width)
    incoming[0, me] = outgoing[0, me]

    load_rows.wait()
    table = a_buf.reshape(cx * (cy + 2 * PAD), cz)
    column = iota((8, width), 1) - iota((8, width), 0)

    def fetch(t, slot):
        places = rows_s.at[t]
        for j in range(width):
            at = places[j]
            picked[slot, j // 8, j % 8 : j % 8 + 1, :] = table[pl.ds(at, 1), :]

    def pick(t, slot):
        lanes = jnp.broadcast_to(lanes_v[pl.ds(t, 1), :], (8, width))
        out = jnp.zeros((8, width), F32)
        for m in range(width // 8):
            got = jnp.take_along_axis(picked[slot, m], lanes, axis=1)
            out = jnp.where(column == 8 * m, got, out)
        values[pl.ds(t, 1), :] = jnp.sum(out, axis=0, keepdims=True)

    def gather(t, carry):
        pick(t - 1, (t - 1) % 2)
        fetch(t, t % 2)
        return carry

    fetch(0, 0)
    early = tiles * EARLY // 64
    lax.fori_loop(1, early, gather, 0)

    pl.semaphore_wait(barrier, devices - 1)
    started = [x_copies(0, a_buf) + yz_copies(0)]
    start_x(started[0])
    for c in started[0][2:]:
        c.start()
    others(lambda o, to, where: tile_copy(0, o, to, where).start())
    lax.fori_loop(early, tiles, gather, 0)
    pick(tiles - 1, (tiles - 1) % 2)
    load_coef.wait()
    total = placed(((first, parts[2]), (second, values[...] * coef[...])))
    outgoing[1] = total.reshape(devices, 8, width)
    others(lambda o, to, where: tile_copy(1, o, to, where).start())
    incoming[1, me] = outgoing[1, me]

    third(a_buf)
    load_d.wait()

    def invert(x, carry):
        inv[x] = 1.0 / (6.0 + inv[x])
        return carry

    lax.fori_loop(0, cx, invert, 0, unroll=4)

    load_s.wait()

    save_edges = [
        local(zsum.at[0], new_p.at[0], 11),
        local(zsum.at[cx - 1], new_p.at[cx - 1], 12),
    ]
    saves = list(save_edges)

    def sweep(it, cur, nxt):
        last = it == ITERS - 1
        for c in started[it]:
            c.wait_recv()
        if 0 < it < ITERS - 1:
            for c in started[it - 1][:2]:
                c.wait_send()

        def rows(x, carry):
            cur[x, pl.ds(PAD - 1, 1), :] = hy[it, 0, pl.ds(x, 1), :]
            cur[x, pl.ds(PAD + cy, 1), :] = hy[it, 1, pl.ds(x, 1), :]
            return carry

        lax.fori_loop(0, cx, rows, 0, unroll=8)
        if nfz > 2:
            hz[it, 0] = jnp.where(even, hz[it, 0], hz[it, 1])

        def plane(x, half, below, mid, above, edges):
            y0 = pl.multiple_of(half * band, band)
            span = pl.ds(y0, band)
            edge = pltpu.roll(edges, (2 * cz - 2 * x) - half * (2 * cx), 1)
            total = zsum[x, span, :] + jnp.where(ends, edge, 0.0)
            total = total + cur[x, pl.ds(y0 + (PAD - 1), band), :]
            total = total + cur[x, pl.ds(y0 + (PAD + 1), band), :]
            new = (total + below + above + src[x, span, :]) * inv[x, span, :]
            if last:
                zsum[x, span, :] = new
            else:
                nxt[x, pl.ds(y0 + PAD, band), :] = new

        def at(x, half):
            return cur[x, pl.ds(pl.multiple_of(half * band, band) + PAD, band), :]

        def outer(half, carry):
            span = pl.ds(pl.multiple_of(half * band, band), band)
            edges = hz[it, 0]
            plane(0, half, hx[it, 0, span, :], at(0, half), at(1, half), edges)
            plane(cx - 1, half, at(cx - 2, half), at(cx - 1, half), hx[it, 1, span, :], edges)
            return carry

        for half in range(halves):
            outer(half, 0)
        if last:
            save_edges[0].start()
            save_edges[1].start()
        if not last:
            started.append(x_copies(it + 1, nxt))
            start_x(started[-1])

        def inner(half, carry):
            edges = hz[it, 0]
            below, mid = at(0, half), at(1, half)
            for x in range(1, cx - 1):
                above = at(x + 1, half)
                plane(x, half, below, mid, above, edges)
                below, mid = mid, above
            return carry

        if last:
            for half in range(halves):
                inner(half, 0)
                rows_of = pl.ds(half * band, band)
                save = local(zsum.at[inside, rows_of], new_p.at[inside, rows_of], half)
                save.start()
                saves.append(save)
        else:
            lax.fori_loop(0, halves, inner, 0)
            more = yz_copies(it + 1)
            send_rows(it + 1, nxt)
            for c in more[1:3]:
                c.start()
            pack_third(it + 1, nxt)
            for c in more[:1] + more[3:]:
                c.start()
            started[-1] = started[-1] + more

    slots = devices * CAP
    lines = devices * 8

    def prepare():
        for half in range(2):
            others(lambda o, to, where: tile_copy(half, o, to, where).wait_recv())
        load_lists.wait()
        low = incoming[0].reshape(lines, width)
        high = incoming[1].reshape(lines, width)
        row = iota((lines, slots), 0)
        col = iota((lines, slots), 1)
        home = (row // 8) * CAP + row % CAP
        lower = row % 8 < CAP
        take = (ones_where((home == col) & lower), ones_where((home == col) & (row % 8 >= CAP)))
        for half, block in ((0, low), (1, high)):
            turned = block.T
            for odd in range(2):
                c = 2 * half + odd
                scaled = turned if c == 3 else turned * SCALE
                hi, lo = split2(scaled)
                span = pl.ds(c * width, width)
                tab[span, 0:slots] = mm(hi, take[odd]).astype(BF16)
                tab[span, slots : 2 * slots] = mm(lo, take[odd]).astype(BF16)
        here = ones_where(low < 0.5 * FAR)
        row = iota((slots, lines), 0)
        col = iota((slots, lines), 1)
        home = (col // 8) * CAP + col % CAP
        lower = col % 8 < CAP
        prefix = mm(ones_where((home <= row) & lower), here)
        there = mm(ones_where((home == row) & lower), here)
        place = jnp.where(there > 0.5, prefix - 1.0, -1.0)
        pos[:, 0:width] = place
        pos[:, width : 2 * width] = place
        count = prefix[slots - 1 : slots, 0:1]
        entry = lists[...].astype(F32)
        rest = entry - jnp.floor(entry / count) * count
        rest = jnp.where(rest < 0.0, rest + count, rest)
        want[...] = jnp.where(rest >= count, rest - count, rest)
        load_nodes.wait()

    neigh = lists.shape[0]

    def gauss(block, carry):
        span = pl.ds(pl.multiple_of(block * NODE_BLOCK, NODE_BLOCK), NODE_BLOCK)
        here = [nodes[c : c + 1, span] * SCALE for c in range(3)]
        total = jnp.zeros((8, NODE_BLOCK), F32)
        for k in range(neigh):
            hot = ones_where(pos[...] == want[k : k + 1, span])
            hot = jnp.concatenate([hot, hot], axis=0)
            got = mm(tab[...], hot)
            far = None
            for c in range(3):
                gap = got[c * width : (c + 1) * width] - here[c]
                far = gap * gap if far is None else far + gap * gap
            term = jnp.exp2(-far) * got[3 * width : 4 * width]
            total = total + jnp.sum(term.reshape(width // 8, 8, NODE_BLOCK), axis=0)
        done = jnp.sum(total, axis=0, keepdims=True)
        for h in range(NODE_BLOCK // 128):
            loads[pl.ds(block * (NODE_BLOCK // 128) + h, 1), :] = done[:, h * 128 : (h + 1) * 128]
        return carry

    bufs = (a_buf, b_buf)
    for it in range(ITERS):
        if it == ITERS - 1:
            for group in started[:-1]:
                for c in group[2:]:
                    c.wait_send()
            for c in started[-2][:2] + started[-1]:
                c.wait_send()
            for half in range(2):
                others(lambda o, to, where: tile_copy(half, o, to, where).wait_send())
        sweep(it, bufs[it % 2], bufs[(it + 1) % 2])
        if it == 1:
            prepare()
        if it < ITERS - 1:
            lax.fori_loop(gauss_bounds[it], gauss_bounds[it + 1], gauss, 0)
    for c in saves:
        c.wait()


def copy_kernel(parts, p_any, loads_any, p_out, loads_out, held, held_loads, sem_in, sem_out):
    depth = p_any.shape[0] // parts
    moves = []
    for i in range(parts):
        span = pl.ds(i * depth, depth)
        moves.append(
            (
                pltpu.make_async_copy(p_any.at[span], held.at[span], sem_in.at[i]),
                pltpu.make_async_copy(held.at[span], p_out.at[span], sem_out.at[i]),
            )
        )
    moves.append(
        (
            pltpu.make_async_copy(loads_any, held_loads, sem_in.at[parts]),
            pltpu.make_async_copy(held_loads, loads_out, sem_out.at[parts]),
        )
    )
    for into, _ in moves:
        into.start()
    for into, out in moves:
        into.wait()
        out.start()
    for _, out in moves:
        out.wait()


def on_device(
    sizes,
    pressure, source, diag_shift, iface_cells, iface_coef, iface_xyz, node_xyz, owners, node_lists,
):
    nfx, nfy, nfz = sizes
    devices = nfx * nfy * nfz
    tiles = owners.shape[0]
    width = iface_coef.shape[0] // tiles
    cx, cy, cz = pressure.shape
    nodes, neigh = node_lists.shape
    vmem = pl.BlockSpec(memory_space=pltpu.VMEM)
    hbm = pl.BlockSpec(memory_space=pltpu.HBM)
    slots = devices * CAP
    blocks = nodes // NODE_BLOCK
    bounds = [blocks * i // 8 for i in (0, 0, 4, 8)]
    dma = pltpu.SemaphoreType.DMA

    def space(*shape, dtype=F32):
        return pltpu.VMEM(shape, dtype)

    new_p, loads = pl.pallas_call(
        functools.partial(main_kernel, sizes, bounds),
        out_shape=(
            jax.ShapeDtypeStruct((cx, cy, cz), F32),
            jax.ShapeDtypeStruct((nodes // 128, 128), F32),
        ),
        in_specs=[hbm] * 9,
        out_specs=(hbm, vmem),
        scratch_shapes=[
            space(cx, cy + 2 * PAD, cz),
            space(cx, cy + 2 * PAD, cz),
            space(cx, cy, cz),
            space(cx, cy, cz),
            space(cx, cy, cz),
            space(ITERS, 2, cy, cz),
            space(ITERS, 2, cx, cz),
            space(ITERS, 2, 2 * cx * cy // cz, cz),
            space(ITERS, 2, cx, cz),
            space(ITERS, 2 * cx * cy // cz, cz),
            space(2 * cz, cz, dtype=BF16),
            space(tiles, width, dtype=jnp.int32),
            space(tiles, width, dtype=jnp.int32),
            space(tiles, width, dtype=jnp.int32),
            pltpu.SMEM((tiles, width), jnp.int32),
            space(tiles, width),
            space(3, tiles * width),
            space(1, tiles, dtype=jnp.int32),
            space(3, nodes),
            space(neigh, nodes, dtype=jnp.int32),
            space(2, width // 8, 8, width),
            space(3, tiles, width),
            space(tiles, width),
            space(2, devices, 8, width),
            space(2, devices, 8, width),
            space(4 * width, 2 * slots, dtype=BF16),
            space(slots, NODE_BLOCK),
            space(neigh, nodes),
            dma((13,)),
            dma((ITERS, 2)), dma((ITERS, 2)),
            dma((ITERS, 2)), dma((ITERS, 2)),
            dma((ITERS, 2)), dma((ITERS, 2)),
            dma((2, devices)), dma((2, devices)),
        ],
        compiler_params=pltpu.CompilerParams(
            collective_id=0, has_side_effects=True, vmem_limit_bytes=56 * 1024 * 1024
        ),
        name="sweeps",
    )(
        pressure,
        source,
        diag_shift,
        iface_cells.reshape(tiles, width),
        iface_coef.reshape(tiles, width),
        iface_xyz,
        owners.reshape(1, tiles),
        node_xyz,
        node_lists.T,
    )
    pieces = 4
    new_p, loads = pl.pallas_call(
        functools.partial(copy_kernel, pieces),
        out_shape=(
            jax.ShapeDtypeStruct((cx, cy, cz), F32),
            jax.ShapeDtypeStruct((nodes // 128, 128), F32),
        ),
        in_specs=[hbm, hbm],
        out_specs=(hbm, hbm),
        scratch_shapes=[
            space(cx, cy, cz),
            space(nodes // 128, 128),
            dma((pieces + 1,)),
            dma((pieces + 1,)),
        ],
        compiler_params=pltpu.CompilerParams(vmem_limit_bytes=56 * 1024 * 1024),
        name="place",
    )(new_p, loads)
    return new_p, loads.reshape(nodes)


def solution(mesh):
    sizes = tuple(mesh.shape[a] for a in ("fx", "fy", "fz"))
    cells = P("fx", "fy", "fz")
    flat = P(("fx", "fy", "fz"))
    return jax.shard_map(
        functools.partial(on_device, sizes),
        mesh=mesh,
        in_specs=(
            cells, cells, cells, flat, flat,
            P(None, ("fx", "fy", "fz")), P(None, ("fx", "fy", "fz")), flat,
            P(("fx", "fy", "fz"), None),
        ),
        out_specs=(cells, flat),
        check_vma=False,
    )
```

```python
import functools
import math

import jax
import jax.numpy as jnp
from jax import lax
from jax.experimental import pallas as pl
from jax.experimental.pallas import tpu as pltpu
from jax.sharding import PartitionSpec as P

ITERS = 4
CAP = 4
GAUSS_RATE = 0.5
SCALE = math.sqrt(GAUSS_RATE * math.log2(math.e))
FAR = 1.0e6
NODE_BLOCK = 256
PAD = 8
MESH = pl.DeviceIdType.MESH
F32 = jnp.float32
BF16 = jnp.bfloat16
EARLY = 28


def split2(x):
    hi = x.astype(BF16)
    return hi, (x - hi.astype(F32)).astype(BF16)


def split3(x):
    hi = x.astype(BF16)
    rest = x - hi.astype(F32)
    mid = rest.astype(BF16)
    return hi, mid, (rest - mid.astype(F32)).astype(BF16)


def mm(a, b):
    return jnp.dot(a, b, preferred_element_type=F32)


def iota(shape, dim):
    return lax.broadcasted_iota(jnp.int32, shape, dim)


def ones_where(mask):
    return jnp.where(mask, 1.0, 0.0).astype(BF16)


def main_kernel(
    sizes, gauss_bounds,
    p_any, s_any, d_any, cells_any, coef_any, xyz_any, own_any, nodes_any, lists_any,
    new_p, loads,
    a_buf, b_buf, src, inv, zsum, hx, hy, hz, ys, zs, shift,
    cells, lanes_v, rows_v, rows_s, coef, xyz, own_v, nodes, lists,
    picked, parts, values, outgoing, incoming, tab, pos, want,
    load_sem, x_send, x_recv, y_send, y_recv, z_send, z_recv, t_send, t_recv,
):
    nfx, nfy, nfz = sizes
    devices = nfx * nfy * nfz
    cx, cy, cz = src.shape
    tiles, width = coef.shape
    bx, by, bz = lax.axis_index("fx"), lax.axis_index("fy"), lax.axis_index("fz")
    me = (bx * nfy + by) * nfz + bz
    body = pl.ds(PAD, cy)

    def local(a, b, k):
        return pltpu.make_async_copy(a, b, load_sem.at[k])

    tx = [(bx + d) % nfx for d in range(nfx)]
    ty = [(by + d) % nfy for d in range(nfy)]
    tz = [(bz + d) % nfz for d in range(nfz)]
    x_next, x_prev = (tx[1 % nfx], by, bz), (tx[nfx - 1], by, bz)
    y_next, y_prev = (bx, ty[1 % nfy], bz), (bx, ty[nfy - 1], bz)
    z_next, z_prev = (bx, by, tz[1 % nfz]), (bx, by, tz[nfz - 1])
    inside = pl.ds(1, cx - 2)
    load_low = local(p_any.at[0], a_buf.at[0, body], 0)
    load_high = local(p_any.at[cx - 1], a_buf.at[cx - 1, body], 1)
    load_p = local(p_any.at[inside], a_buf.at[inside, body, :], 2)
    load_cells = local(cells_any, cells, 3)
    load_own = local(own_any, own_v, 4)
    load_xyz = local(xyz_any, xyz, 5)
    load_d = local(d_any, inv, 6)
    load_s = local(s_any, src, 7)
    load_coef = local(coef_any, coef, 8)
    load_nodes = local(nodes_any, nodes, 9)
    load_lists = local(lists_any, lists, 10)
    for c in (
        load_low, load_high, load_p, load_cells, load_own, load_xyz,
        load_d, load_s, load_coef, load_nodes, load_lists,
    ):
        c.start()

    def others(act):
        def inner(x_to, first, base):
            for dy in range(nfy):
                for dz in range(nfz):
                    if first and dy == 0 and dz == 0:
                        continue
                    to = (x_to * nfy + ty[dy]) * nfz + tz[dz]
                    act(base + dy * nfz + dz, to, (x_to, ty[dy], tz[dz]))

        inner(tx[0], True, 0)

        def step(d, carry):
            inner((bx + d) % nfx, False, d * (nfy * nfz))
            return carry

        lax.fori_loop(1, nfx, step, 0)

    barrier = pltpu.get_barrier_semaphore()
    others(
        lambda o, to, where: pl.semaphore_signal(
            barrier, inc=1, device_id=where, device_id_type=MESH
        )
    )

    def remote(a, b, ss, rs, device):
        return pltpu.make_async_remote_copy(
            src_ref=a, dst_ref=b, send_sem=ss, recv_sem=rs, device_id=device, device_id_type=MESH
        )

    def tile_copy(half, o, to, where):
        return remote(
            outgoing.at[half, to], incoming.at[half, me],
            t_send.at[half, o], t_recv.at[half, o], where,
        )

    def x_copies(it, buf):
        return [
            remote(buf.at[cx - 1, body], hx.at[it, 0], x_send.at[it, 0], x_recv.at[it, 0], x_next),
            remote(buf.at[0, body], hx.at[it, 1], x_send.at[it, 1], x_recv.at[it, 1], x_prev),
        ]

    def start_x(copies):
        @pl.when(bx == 0)
        def _():
            copies[1].start()
            copies[0].start()

        @pl.when(bx != 0)
        def _():
            copies[0].start()
            copies[1].start()

    def yz_copies(it):
        made = [
            remote(zs.at[it], hz.at[it, 0], z_send.at[it, 0], z_recv.at[it, 0], z_next),
            remote(ys.at[it, 1], hy.at[it, 0], y_send.at[it, 0], y_recv.at[it, 0], y_next),
            remote(ys.at[it, 0], hy.at[it, 1], y_send.at[it, 1], y_recv.at[it, 1], y_prev),
        ]
        if nfz > 2:
            made.append(
                remote(zs.at[it], hz.at[it, 1], z_send.at[it, 1], z_recv.at[it, 1], z_prev)
            )
        return made

    halves = cz // (2 * cx)
    band = cy // halves
    lane = iota((band, cz), 1)
    pair = lax.shift_right_logical(lane, 1)
    even = lane % 2 == 0
    ends = (lane == 0) | (lane == cz - 1)

    def send_rows(it, buf):
        def one(x, carry):
            ys[it, 0, pl.ds(x, 1), :] = buf[x, pl.ds(PAD, 1), :]
            ys[it, 1, pl.ds(x, 1), :] = buf[x, pl.ds(PAD + cy - 1, 1), :]
            return carry

        lax.fori_loop(0, cx, one, 0, unroll=8)

    def pack_only(half, buf, packed):
        y0 = pl.multiple_of(half * band, band)
        for x in range(cx):
            moved = pltpu.roll(buf[x, pl.ds(y0 + PAD, band), :], half * (2 * cx) + (2 * x + 1), 1)
            packed = jnp.where(pair == x + half * cx, moved, packed)
        return packed

    def third_only(half, buf):
        y0 = pl.multiple_of(half * band, band)
        hi, lo = split2(buf[:, pl.ds(y0 + PAD, band), :].reshape(cx * band, cz))
        near = mm(jnp.concatenate([hi, lo], axis=1), shift[...])
        zsum[:, pl.ds(y0, band), :] = near.reshape(cx, band, cz)

    def store_packed(it, packed):
        zs[it] = jnp.where(even, packed, pltpu.roll(packed, cz - 2, 1))

    def pack(it, buf):
        packed = jnp.zeros((band, cz), F32)
        packed = lax.fori_loop(0, halves, lambda half, z: pack_only(half, buf, z), packed)
        store_packed(it, packed)

    def third(buf):
        lax.fori_loop(0, halves, lambda half, z: (third_only(half, buf), z)[1], 0)

    def pack_third(it, buf):
        def both(half, packed):
            third_only(half, buf)
            return pack_only(half, buf, packed)

        store_packed(it, lax.fori_loop(0, halves, both, jnp.zeros((band, cz), F32)))

    apart = jnp.abs(iota((cz, cz), 0) - iota((cz, cz), 1))
    for part in range(2):
        shift[part * cz : (part + 1) * cz, :] = ones_where(apart == 1)

    load_low.wait()
    load_high.wait()
    load_p.wait()
    send_rows(0, a_buf)
    pack(0, a_buf)
    load_cells.wait()
    flat = cells[...]
    row_of = lax.shift_right_logical(flat, cz.bit_length() - 1)
    plane_of = lax.shift_right_logical(row_of, cy.bit_length() - 1)
    rows_v[...] = row_of + plane_of * (2 * PAD) + PAD
    lanes_v[...] = jnp.bitwise_and(flat, cz - 1)

    load_rows = pltpu.make_async_copy(rows_v, rows_s, load_sem.at[3])
    load_rows.start()

    load_own.wait()
    own = own_v[...]
    mine = iota((devices, tiles), 0) == own
    before = ones_where(iota((tiles, tiles), 0) < iota((tiles, tiles), 1))
    earlier = mm(ones_where(mine), before)
    rank = jnp.sum(jnp.where(mine, earlier, 0.0), axis=0, keepdims=True)
    target = own * CAP + rank.astype(jnp.int32)
    line = iota((devices * 8, tiles), 0)
    at_slot = (line // 8) * CAP + line % CAP == target
    low_rows = line % 8 < CAP
    first = ones_where(at_slot & low_rows)
    second = ones_where(at_slot & jnp.logical_not(low_rows))
    filled = mm(first, jnp.ones((tiles, width), BF16))

    load_xyz.wait()

    def spread(t, carry):
        base = pl.multiple_of(t * width, width)
        for c in range(3):
            parts[c, pl.ds(t, 1), :] = xyz[c : c + 1, pl.ds(base, width)]
        return carry

    lax.fori_loop(0, tiles, spread, 0, unroll=8)

    def placed(pairs):
        total = None
        for sel, block in pairs:
            for piece in split3(block):
                term = mm(sel, piece)
                total = term if total is None else total + term
        return total

    total = placed(((first, parts[0]), (second, parts[1])))
    empty = (iota(filled.shape, 0) % 8 < CAP) & (filled < 0.5)
    outgoing[0] = jnp.where(empty, FAR, total).reshape(devices, 8, width)
    incoming[0, me] = outgoing[0, me]

    load_rows.wait()
    table = a_buf.reshape(cx * (cy + 2 * PAD), cz)
    column = iota((8, width), 1) - iota((8, width), 0)

    def fetch(t, slot):
        places = rows_s.at[t]
        for j in range(width):
            at = places[j]
            picked[slot, j // 8, j % 8 : j % 8 + 1, :] = table[pl.ds(at, 1), :]

    def pick(t, slot):
        lanes = jnp.broadcast_to(lanes_v[pl.ds(t, 1), :], (8, width))
        out = jnp.zeros((8, width), F32)
        for m in range(width // 8):
            got = jnp.take_along_axis(picked[slot, m], lanes, axis=1)
            out = jnp.where(column == 8 * m, got, out)
        values[pl.ds(t, 1), :] = jnp.sum(out, axis=0, keepdims=True)

    def gather(t, carry):
        pick(t - 1, (t - 1) % 2)
        fetch(t, t % 2)
        return carry

    fetch(0, 0)
    early = tiles * EARLY // 64
    lax.fori_loop(1, early, gather, 0)

    pl.semaphore_wait(barrier, devices - 1)
    started = [x_copies(0, a_buf) + yz_copies(0)]
    start_x(started[0])
    for c in started[0][2:]:
        c.start()
    others(lambda o, to, where: tile_copy(0, o, to, where).start())
    lax.fori_loop(early, tiles, gather, 0)
    pick(tiles - 1, (tiles - 1) % 2)
    load_coef.wait()
    total = placed(((first, parts[2]), (second, values[...] * coef[...])))
    outgoing[1] = total.reshape(devices, 8, width)
    others(lambda o, to, where: tile_copy(1, o, to, where).start())
    incoming[1, me] = outgoing[1, me]

    third(a_buf)
    load_d.wait()

    def invert(x, carry):
        inv[x] = 1.0 / (6.0 + inv[x])
        return carry

    lax.fori_loop(0, cx, invert, 0, unroll=4)

    load_s.wait()

    save_edges = [
        local(zsum.at[0], new_p.at[0], 11),
        local(zsum.at[cx - 1], new_p.at[cx - 1], 12),
    ]
    saves = list(save_edges)

    def sweep(it, cur, nxt):
        last = it == ITERS - 1
        for c in started[it]:
            c.wait_recv()
        if 0 < it < ITERS - 1:
            for c in started[it - 1][:2]:
                c.wait_send()

        def rows(x, carry):
            cur[x, pl.ds(PAD - 1, 1), :] = hy[it, 0, pl.ds(x, 1), :]
            cur[x, pl.ds(PAD + cy, 1), :] = hy[it, 1, pl.ds(x, 1), :]
            return carry

        lax.fori_loop(0, cx, rows, 0, unroll=8)
        if nfz > 2:
            hz[it, 0] = jnp.where(even, hz[it, 0], hz[it, 1])

        def plane(x, half, below, mid, above, edges):
            y0 = pl.multiple_of(half * band, band)
            span = pl.ds(y0, band)
            edge = pltpu.roll(edges, (2 * cz - 2 * x) - half * (2 * cx), 1)
            total = zsum[x, span, :] + jnp.where(ends, edge, 0.0)
            total = total + cur[x, pl.ds(y0 + (PAD - 1), band), :]
            total = total + cur[x, pl.ds(y0 + (PAD + 1), band), :]
            new = (total + below + above + src[x, span, :]) * inv[x, span, :]
            if last:
                zsum[x, span, :] = new
            else:
                nxt[x, pl.ds(y0 + PAD, band), :] = new

        def at(x, half):
            return cur[x, pl.ds(pl.multiple_of(half * band, band) + PAD, band), :]

        def outer(half, carry):
            span = pl.ds(pl.multiple_of(half * band, band), band)
            edges = hz[it, 0]
            plane(0, half, hx[it, 0, span, :], at(0, half), at(1, half), edges)
            plane(cx - 1, half, at(cx - 2, half), at(cx - 1, half), hx[it, 1, span, :], edges)
            return carry

        for half in range(halves):
            outer(half, 0)
        if last:
            save_edges[0].start()
            save_edges[1].start()
        if not last:
            started.append(x_copies(it + 1, nxt))
            start_x(started[-1])

        def inner(half, carry):
            edges = hz[it, 0]
            below, mid = at(0, half), at(1, half)
            for x in range(1, cx - 1):
                above = at(x + 1, half)
                plane(x, half, below, mid, above, edges)
                below, mid = mid, above
            return carry

        if last:
            for half in range(halves):
                inner(half, 0)
                rows_of = pl.ds(half * band, band)
                save = local(zsum.at[inside, rows_of], new_p.at[inside, rows_of], half)
                save.start()
                saves.append(save)
        else:
            lax.fori_loop(0, halves, inner, 0)
            more = yz_copies(it + 1)
            send_rows(it + 1, nxt)
            for c in more[1:3]:
                c.start()
            pack_third(it + 1, nxt)
            for c in more[:1] + more[3:]:
                c.start()
            started[-1] = started[-1] + more

    slots = devices * CAP
    lines = devices * 8

    def prepare():
        for half in range(2):
            others(lambda o, to, where: tile_copy(half, o, to, where).wait_recv())
        load_lists.wait()
        low = incoming[0].reshape(lines, width)
        high = incoming[1].reshape(lines, width)
        row = iota((lines, slots), 0)
        col = iota((lines, slots), 1)
        home = (row // 8) * CAP + row % CAP
        lower = row % 8 < CAP
        take = (ones_where((home == col) & lower), ones_where((home == col) & (row % 8 >= CAP)))
        for half, block in ((0, low), (1, high)):
            turned = block.T
            for odd in range(2):
                c = 2 * half + odd
                scaled = turned if c == 3 else turned * SCALE
                hi, lo = split2(scaled)
                span = pl.ds(c * width, width)
                tab[span, 0:slots] = mm(hi, take[odd]).astype(BF16)
                tab[span, slots : 2 * slots] = mm(lo, take[odd]).astype(BF16)
        here = ones_where(low < 0.5 * FAR)
        row = iota((slots, lines), 0)
        col = iota((slots, lines), 1)
        home = (col // 8) * CAP + col % CAP
        lower = col % 8 < CAP
        prefix = mm(ones_where((home <= row) & lower), here)
        there = mm(ones_where((home == row) & lower), here)
        place = jnp.where(there > 0.5, prefix - 1.0, -1.0)
        pos[:, 0:width] = place
        pos[:, width : 2 * width] = place
        count = prefix[slots - 1 : slots, 0:1]
        entry = lists[...].astype(F32)
        rest = entry - jnp.floor(entry / count) * count
        rest = jnp.where(rest < 0.0, rest + count, rest)
        want[...] = jnp.where(rest >= count, rest - count, rest)
        load_nodes.wait()

    neigh = lists.shape[0]

    def gauss(block, carry):
        span = pl.ds(pl.multiple_of(block * NODE_BLOCK, NODE_BLOCK), NODE_BLOCK)
        here = [nodes[c : c + 1, span] * SCALE for c in range(3)]
        total = jnp.zeros((8, NODE_BLOCK), F32)
        for k in range(neigh):
            hot = ones_where(pos[...] == want[k : k + 1, span])
            hot = jnp.concatenate([hot, hot], axis=0)
            got = mm(tab[...], hot)
            far = None
            for c in range(3):
                gap = got[c * width : (c + 1) * width] - here[c]
                far = gap * gap if far is None else far + gap * gap
            term = jnp.exp2(-far) * got[3 * width : 4 * width]
            total = total + jnp.sum(term.reshape(width // 8, 8, NODE_BLOCK), axis=0)
        done = jnp.sum(total, axis=0, keepdims=True)
        for h in range(NODE_BLOCK // 128):
            loads[pl.ds(block * (NODE_BLOCK // 128) + h, 1), :] = done[:, h * 128 : (h + 1) * 128]
        return carry

    bufs = (a_buf, b_buf)
    for it in range(ITERS):
        sweep(it, bufs[it % 2], bufs[(it + 1) % 2])
        if it == 1:
            prepare()
        if it < ITERS - 1:
            lax.fori_loop(gauss_bounds[it], gauss_bounds[it + 1], gauss, 0)
    for group in started[:-1]:
        for c in group[2:]:
            c.wait_send()
    for c in started[-2][:2] + started[-1]:
        c.wait_send()
    for half in range(2):
        others(lambda o, to, where: tile_copy(half, o, to, where).wait_send())
    for c in saves:
        c.wait()


def copy_kernel(parts, p_any, loads_any, p_out, loads_out, held, held_loads, sem_in, sem_out):
    depth = p_any.shape[0] // parts
    moves = []
    for i in range(parts):
        span = pl.ds(i * depth, depth)
        moves.append(
            (
                pltpu.make_async_copy(p_any.at[span], held.at[span], sem_in.at[i]),
                pltpu.make_async_copy(held.at[span], p_out.at[span], sem_out.at[i]),
            )
        )
    moves.append(
        (
            pltpu.make_async_copy(loads_any, held_loads, sem_in.at[parts]),
            pltpu.make_async_copy(held_loads, loads_out, sem_out.at[parts]),
        )
    )
    for into, _ in moves:
        into.start()
    for into, out in moves:
        into.wait()
        out.start()
    for _, out in moves:
        out.wait()


def on_device(
    sizes,
    pressure, source, diag_shift, iface_cells, iface_coef, iface_xyz, node_xyz, owners, node_lists,
):
    nfx, nfy, nfz = sizes
    devices = nfx * nfy * nfz
    tiles = owners.shape[0]
    width = iface_coef.shape[0] // tiles
    cx, cy, cz = pressure.shape
    nodes, neigh = node_lists.shape
    vmem = pl.BlockSpec(memory_space=pltpu.VMEM)
    hbm = pl.BlockSpec(memory_space=pltpu.HBM)
    slots = devices * CAP
    blocks = nodes // NODE_BLOCK
    bounds = [blocks * i // 8 for i in (0, 0, 4, 8)]
    dma = pltpu.SemaphoreType.DMA

    def space(*shape, dtype=F32):
        return pltpu.VMEM(shape, dtype)

    new_p, loads = pl.pallas_call(
        functools.partial(main_kernel, sizes, bounds),
        out_shape=(
            jax.ShapeDtypeStruct((cx, cy, cz), F32),
            jax.ShapeDtypeStruct((nodes // 128, 128), F32),
        ),
        in_specs=[hbm] * 9,
        out_specs=(hbm, vmem),
        scratch_shapes=[
            space(cx, cy + 2 * PAD, cz),
            space(cx, cy + 2 * PAD, cz),
            space(cx, cy, cz),
            space(cx, cy, cz),
            space(cx, cy, cz),
            space(ITERS, 2, cy, cz),
            space(ITERS, 2, cx, cz),
            space(ITERS, 2, 2 * cx * cy // cz, cz),
            space(ITERS, 2, cx, cz),
            space(ITERS, 2 * cx * cy // cz, cz),
            space(2 * cz, cz, dtype=BF16),
            space(tiles, width, dtype=jnp.int32),
            space(tiles, width, dtype=jnp.int32),
            space(tiles, width, dtype=jnp.int32),
            pltpu.SMEM((tiles, width), jnp.int32),
            space(tiles, width),
            space(3, tiles * width),
            space(1, tiles, dtype=jnp.int32),
            space(3, nodes),
            space(neigh, nodes, dtype=jnp.int32),
            space(2, width // 8, 8, width),
            space(3, tiles, width),
            space(tiles, width),
            space(2, devices, 8, width),
            space(2, devices, 8, width),
            space(4 * width, 2 * slots, dtype=BF16),
            space(slots, NODE_BLOCK),
            space(neigh, nodes),
            dma((13,)),
            dma((ITERS, 2)), dma((ITERS, 2)),
            dma((ITERS, 2)), dma((ITERS, 2)),
            dma((ITERS, 2)), dma((ITERS, 2)),
            dma((2, devices)), dma((2, devices)),
        ],
        compiler_params=pltpu.CompilerParams(
            collective_id=0, has_side_effects=True, vmem_limit_bytes=56 * 1024 * 1024
        ),
        name="sweeps",
    )(
        pressure,
        source,
        diag_shift,
        iface_cells.reshape(tiles, width),
        iface_coef.reshape(tiles, width),
        iface_xyz,
        owners.reshape(1, tiles),
        node_xyz,
        node_lists.T,
    )
    pieces = 8
    new_p, loads = pl.pallas_call(
        functools.partial(copy_kernel, pieces),
        out_shape=(
            jax.ShapeDtypeStruct((cx, cy, cz), F32),
            jax.ShapeDtypeStruct((nodes // 128, 128), F32),
        ),
        in_specs=[hbm, hbm],
        out_specs=(hbm, hbm),
        scratch_shapes=[
            space(cx, cy, cz),
            space(nodes // 128, 128),
            dma((pieces + 1,)),
            dma((pieces + 1,)),
        ],
        compiler_params=pltpu.CompilerParams(vmem_limit_bytes=56 * 1024 * 1024),
        name="place",
    )(new_p, loads)
    return new_p, loads.reshape(nodes)


def solution(mesh):
    sizes = tuple(mesh.shape[a] for a in ("fx", "fy", "fz"))
    cells = P("fx", "fy", "fz")
    flat = P(("fx", "fy", "fz"))
    return jax.shard_map(
        functools.partial(on_device, sizes),
        mesh=mesh,
        in_specs=(
            cells, cells, cells, flat, flat,
            P(None, ("fx", "fy", "fz")), P(None, ("fx", "fy", "fz")), flat,
            P(("fx", "fy", "fz"), None),
        ),
        out_specs=(cells, flat),
        check_vma=False,
    )
```
